32 devices in a mesh: chain: 8 (over z, core), dp: 4 (over y, x).
Axes of the slice: x: 2, y: 2, z: 4, core: 2. Of those that a mesh axis runs over, the one named last changes fastest.
Arguments:
- images_in: float32 [8, 1024, 1024], P('chain', 'dp'), may hold values from -8 to 8
- images_mid: float32 [8, 1024, 1024], P('chain', 'dp'), may hold values from -8 to 8
- images_out: float32 [8, 1024, 1000], P('chain', 'dp'), may hold values from -8 to 8
- ends_in: float32 [2, 1024, 1024], P(None, 'dp'), may hold values from -8 to 8
- ends_mid: float32 [2, 1024, 1024], P(None, 'dp'), may hold values from -8 to 8
- ends_out: float32 [2, 1024, 1000], P(None, 'dp'), may hold values from -8 to 8
- data_pool: bfloat16 [7168, 1024], P('dp'), may hold values from -6 to 6
- batch_rows: int32 [8, 3584], P('chain', 'dp'), may hold values from 0 to 1791
- labels: int32 [8, 3584], P('chain', 'dp'), may hold values from 0 to 999
- climbing: int32 [8], P('chain'), may hold values 0 or 1
Outputs:
- new_in: float32 [8, 1024, 1024], P('chain', 'dp')
- new_mid: float32 [8, 1024, 1024], P('chain', 'dp')
- new_out: float32 [8, 1024, 1000], P('chain', 'dp')
- energies: float32 [8], P('chain')
- arc_share: float32 [8], P('chain')
- bend: float32 [8], P('chain')
The draws below stay inside these ranges and needn't reach their ends.
Inputs may be any that keep to these rules, and one draw needn't show every extreme that they name: batch_rows[i, b] names a row of the pool shard held by dp index b // 896.
All inputs are finite; a program needn't handle non-finite values. No bound on the sum of `climbing` on one device may be relied on, other than what follows from the above.
Results may differ from the reference program's by a relative error of at most 0.0023.
Values may be sent and summed in bfloat16 or wider, within the bound.
A program may use at most 128 MiB of HBM per device.

```python
import jax
import jax.numpy as jnp
from jax import lax

D = 1024
FF = 1024
C = 1000
B_DEV = 896
POOL = 1792
IMAGES = 8
BATCH = 3584
ROWS = 7168


def row_scale(count):
    top = 2.5
    return jnp.exp(jnp.log(top) * jnp.arange(count, dtype=jnp.float32) / (count - 1))


def band_ends(key, tag, shape):
    scale = row_scale(shape[0])[:, None]
    first = jax.random.normal(jax.random.fold_in(key, tag), shape, jnp.float32) * scale
    second = jax.random.normal(jax.random.fold_in(key, tag + 100), shape, jnp.float32) * scale
    return (jnp.clip(first, -7.5, 7.5), jnp.clip(second, -7.5, 7.5))


def band_images(key, tag, shape):
    first, second = band_ends(key, tag, shape)
    scale = row_scale(shape[0])[None, :, None]
    spacing = 1.0 + 2.0 * jnp.arange(IMAGES + 1, dtype=jnp.float32) / IMAGES
    along = jnp.cumsum(spacing)[:IMAGES] / jnp.sum(spacing)
    noise_key = jax.random.fold_in(key, tag + 200)
    noise = 0.03 * jax.random.normal(noise_key, (IMAGES,) + shape, jnp.float32)
    return first[None] + along[:, None, None] * (second - first)[None] + noise * scale


def draw_images_in(key, part):
    return band_images(key, 1, (D, FF))


def draw_images_mid(key, part):
    return band_images(key, 2, (FF, D))


def draw_images_out(key, part):
    return band_images(key, 3, (D, C))


def draw_ends_in(key, part):
    return jnp.stack(band_ends(key, 1, (D, FF)))


def draw_ends_mid(key, part):
    return jnp.stack(band_ends(key, 2, (FF, D)))


def draw_ends_out(key, part):
    return jnp.stack(band_ends(key, 3, (D, C)))


def plant(result, rng, least, high):
    dims = result.shape
    index_at = [jax.random.randint(jax.random.fold_in(rng, axis), (), 0, dims[axis]) for axis in range(len(dims))]
    result = result.at[tuple(index_at)].set(least)
    longest = dims.index(max(dims))
    index_at[longest] = (index_at[longest] + 1) % dims[longest]
    return result.at[tuple(index_at)].set(high)


def steps_of(rng, dims, shards, low, high):
    def one(axis_at, blocks):
        draws = jax.random.uniform(jax.random.fold_in(jax.random.fold_in(rng, 6), axis_at), (blocks,), jnp.float32, low / len(shards), high / len(shards))
        return jnp.repeat(jnp.exp(draws), dims[axis_at] // blocks).reshape((-1,) + (1,) * (len(dims) - axis_at - 1))

    gain = one(*shards[0])
    for cut in shards[1:]:
        gain = gain * one(*cut)
    return gain


def centred(key, dims, width, bound, split=(), kind=jnp.bfloat16):
    factor_of = steps_of(key, dims, split, -0.22, 0.18) if split else 1.0
    values = jax.random.normal(key, dims, jnp.float32) * width * factor_of
    return jnp.minimum(jnp.maximum(values, -bound), bound).astype(kind)


def setup_inputs(seed: int = 0) -> dict:
    seeds = jax.random.split(jax.random.key(seed), 11)
    return {
        "images_in": draw_images_in(jax.random.fold_in(seeds[10], 71), 0),
        "images_mid": draw_images_mid(jax.random.fold_in(seeds[10], 71), 0),
        "images_out": draw_images_out(jax.random.fold_in(seeds[10], 71), 0),
        "ends_in": draw_ends_in(jax.random.fold_in(seeds[10], 71), 0),
        "ends_mid": draw_ends_mid(jax.random.fold_in(seeds[10], 71), 0),
        "ends_out": draw_ends_out(jax.random.fold_in(seeds[10], 71), 0),
        "data_pool": centred(seeds[6], (ROWS, D), 1.0, 6.0, ((0, 4),)),
        "batch_rows": plant(jax.random.randint(seeds[7], (IMAGES, BATCH), 0, POOL), jax.random.fold_in(seeds[7], 1), 0, POOL - 1).astype(jnp.int32),
        "labels": plant(jax.random.randint(seeds[8], (IMAGES, BATCH), 0, C), jax.random.fold_in(seeds[8], 1), 0, C - 1).astype(jnp.int32),
        "climbing": plant((jax.random.randint(seeds[9], (IMAGES,), 0, 4) < 1).astype(jnp.int32), jax.random.fold_in(seeds[9], 1), 0, 1),
    }


SPRING = 0.03
EPS = 1e-06

def silu_slope(pre):
    sig = jax.nn.sigmoid(pre)
    return sig * (1.0 + pre * (1.0 - sig))

def image_terms(packed, data_pool):
    p_in, p_mid, p_out, picks, labs = packed
    w_in = (p_in * D ** (-0.5)).astype(jnp.bfloat16)
    w_mid = (p_mid * FF ** (-0.5)).astype(jnp.bfloat16)
    w_out = (p_out * D ** (-0.5)).astype(jnp.bfloat16)
    owner = (jnp.arange(BATCH, dtype=jnp.int32) // B_DEV).astype(jnp.int32)
    rows = data_pool[owner * POOL + picks]
    pre = jnp.dot(rows, w_in, preferred_element_type=jnp.float32)
    hid = jax.nn.silu(pre).astype(jnp.bfloat16)
    resid = (rows.astype(jnp.float32) + jnp.dot(hid, w_mid, preferred_element_type=jnp.float32)).astype(jnp.bfloat16)
    logits = jnp.dot(resid, w_out, preferred_element_type=jnp.float32)
    target = (labs[:, None] == jnp.arange(C, dtype=jnp.int32)[None, :]).astype(jnp.float32)
    err = logits - target
    norm = 1.0 / (BATCH * C)
    energy = 0.5 * norm * jnp.sum(err * err)
    d_logits = (err * norm).astype(jnp.bfloat16)
    d_resid = jnp.dot(d_logits, w_out.T, preferred_element_type=jnp.float32).astype(jnp.bfloat16)
    d_pre = (jnp.dot(d_resid, w_mid.T, preferred_element_type=jnp.float32) * silu_slope(pre)).astype(jnp.bfloat16)
    g_in = jnp.dot(rows.T, d_pre, preferred_element_type=jnp.float32) * D ** (-0.5)
    g_mid = jnp.dot(hid.T, d_resid, preferred_element_type=jnp.float32) * FF ** (-0.5)
    g_out = jnp.dot(resid.T, d_logits, preferred_element_type=jnp.float32) * D ** (-0.5)
    return (g_in, g_mid, g_out, energy)

def inner(first, second):
    total = jnp.zeros((first[0].shape[0],), jnp.float32)
    for left, right in zip(first, second):
        total = total + lax.optimization_barrier(jnp.sum(left * right, axis=(1, 2)))
    return total

def reference(images_in, images_mid, images_out, ends_in, ends_mid, ends_out, data_pool, batch_rows, labels, climbing):
    g_in, g_mid, g_out, energies = lax.map(lambda packed: image_terms(packed, data_pool), (images_in, images_mid, images_out, batch_rows, labels))
    own = (images_in, images_mid, images_out)
    ends = (ends_in, ends_mid, ends_out)
    grads = (g_in, g_mid, g_out)
    before = tuple((jnp.concatenate([e[0:1], o[:-1]], axis=0) for e, o in zip(ends, own)))
    after = tuple((jnp.concatenate([o[1:], e[1:2]], axis=0) for e, o in zip(ends, own)))
    ahead = tuple((a - o for a, o in zip(after, own)))
    behind = tuple((o - b for o, b in zip(own, before)))
    len_ahead = jnp.sqrt(inner(ahead, ahead) + EPS)
    len_behind = jnp.sqrt(inner(behind, behind) + EPS)
    raw = tuple((a / len_ahead[:, None, None] + b / len_behind[:, None, None] for a, b in zip(ahead, behind)))
    raw_norm = jnp.sqrt(inner(raw, raw) + EPS)
    tau = tuple((r / raw_norm[:, None, None] for r in raw))
    along = inner(grads, tau)
    arc = jnp.cumsum(len_behind)
    band = jnp.sum(len_behind) + len_ahead[-1]
    order = jnp.arange(IMAGES, dtype=jnp.int32)
    target = (order + 1).astype(jnp.float32) / (IMAGES + 1) * band
    coef = jnp.where(climbing == 1, 2.0 * along, along + SPRING * (target - arc) / band)
    force = tuple((-g + coef[:, None, None] * t for g, t in zip(grads, tau)))
    force_len = jnp.sqrt(inner(force, force) + EPS)
    scale = band / (IMAGES + 1) / force_len
    new = tuple((o + scale[:, None, None] * f for o, f in zip(own, force)))
    return (new[0], new[1], new[2], energies, arc / band, 0.5 * raw_norm)
```

```python
import functools

import jax
import jax.numpy as jnp
from jax import lax
from jax.experimental import pallas as pl
from jax.experimental.pallas import tpu as pltpu
from jax.sharding import PartitionSpec as P

SPRING = 0.03
EPS = 1e-06
TILE = 256
LANES = 128
F32 = jnp.float32
BF16 = jnp.bfloat16


def grid_of(count):
    rows = max(k for k in range(1, count + 1) if count % k == 0 and k * k <= count)
    return rows, count // rows


def copies_of(count, chain):
    gy, gx = grid_of(count)
    gather = 2 * (gx - 1) + 2 * (gy - 1) + 2 * (gx - 1) * (gy - 1)
    scatter = (gy - 1) * gx + (gx - 1) * gy + (gx - 1) + (gy - 1)
    return 3 * (gather + scatter) + 2 * (count - 1) + (chain - 1) + 6


def dot_nn(left, right):
    return jnp.dot(left, right, preferred_element_type=F32)


def dot_nt(left, right):
    return lax.dot_general(left, right, (((1,), (1,)), ((), ())), preferred_element_type=F32)


def dot_tn(left, right):
    return lax.dot_general(left, right, (((0,), (0,)), ((), ())), preferred_element_type=F32)


def fold(value):
    part = jnp.sum(value.reshape(value.shape[0] // 8, 8, value.shape[1]), axis=0)
    total = part[:, :LANES]
    for k in range(1, value.shape[1] // LANES):
        total = total + part[:, k * LANES : (k + 1) * LANES]
    return total


def whole(tile):
    return jnp.sum(tile, axis=(0, 1), keepdims=True)


def kernel(
    n,
    c,
    classes,
    p_in,
    p_mid,
    p_out,
    e_in,
    e_mid,
    e_out,
    pool,
    picks,
    labs,
    climb,
    o_in,
    o_mid,
    o_out,
    o_energy,
    o_arc,
    o_bend,
    own,
    edge,
    thin,
    tau,
    wide,
    near,
    before,
    after,
    pool_v,
    hot,
    lab_t,
    rows,
    slope,
    hid,
    resid,
    dlog,
    dres,
    grad,
    from_y,
    from_x,
    last_x,
    last_y,
    sums,
    spans,
    late,
    load_sem,
    send_sem,
    recv_sem,
):
    ci, me = lax.axis_index("chain"), lax.axis_index("dp")
    gy, gx = grid_of(n)
    my, mx = me // gx, lax.rem(me, gx)
    block, width = own.shape[1], own.shape[2]
    depth = n * block
    half = block // 2
    step = min(32, half)
    batch = rows.shape[0]
    tiles = width // TILE
    factor = (depth**-0.5, width**-0.5, depth**-0.5)
    norm = 1.0 / (batch * n * classes)
    counter = [0]

    def remote(src, dst, to):
        k = counter[0]
        counter[0] += 1
        copy = pltpu.make_async_remote_copy(
            src_ref=src,
            dst_ref=dst,
            send_sem=send_sem.at[k],
            recv_sem=recv_sem.at[k],
            device_id=to,
            device_id_type=pl.DeviceIdType.MESH,
        )
        return copy

    def dp_peer(y, x):
        return (ci, y * gx + x)

    def y_at(d):
        return lax.rem(my + d, gy)

    def x_at(d):
        return lax.rem(mx + d, gx)

    barrier = pltpu.get_barrier_semaphore()
    for d in range(1, n):
        pl.semaphore_signal(
            barrier, inc=1, device_id=(ci, lax.rem(me + d, n)), device_id_type=pl.DeviceIdType.MESH
        )
    for d in range(1, c):
        pl.semaphore_signal(
            barrier, inc=1, device_id=(lax.rem(ci + d, c), me), device_id_type=pl.DeviceIdType.MESH
        )

    end = jnp.where(ci == 0, 0, 1)
    loads = [
        pltpu.make_async_copy(p_in.at[0], own.at[0], load_sem.at[0]),
        pltpu.make_async_copy(p_mid.at[0], own.at[1], load_sem.at[1]),
        pltpu.make_async_copy(p_out.at[0], thin.at[0], load_sem.at[2]),
        pltpu.make_async_copy(pool, pool_v, load_sem.at[3]),
        pltpu.make_async_copy(e_in.at[end], edge.at[0], load_sem.at[4]),
        pltpu.make_async_copy(e_mid.at[end], edge.at[1], load_sem.at[5]),
        pltpu.make_async_copy(e_out.at[end], thin.at[1], load_sem.at[6]),
    ]
    for load in loads:
        load.start()

    def widened(into, thin_at):
        pad = classes // LANES * LANES

        def body(r, _):
            at = pl.ds(pl.multiple_of(r * step, step), step)
            if pad < width:
                into[at, pad:] = jnp.zeros((step, width - pad), F32)
            into[at, :classes] = thin[thin_at, at, :]
            return 0

        lax.fori_loop(0, block // step, body, 0)

    def lowered(m):
        def body(r, _):
            off = pl.multiple_of(r * step, step)
            value = own[m, pl.ds(off, step), :]
            wide[m, pl.ds(pl.multiple_of(me * block + off, step), step), :] = (
                value * factor[m]
            ).astype(BF16)
            near[m, pl.ds(off, step), :] = value.astype(BF16)
            return 0

        lax.fori_loop(0, block // step, body, 0)

    for m in range(3):
        loads[m].wait()
        if m == 2:
            widened(own.at[2], 0)
        lowered(m)
    pl.semaphore_wait(barrier, n - 1 + c - 1)

    def piece(ref, m, index, h):
        return ref.at[m, pl.ds(pl.multiple_of(index * block + h * half, half), half), :]

    started = []

    def begin(copy):
        copy.start()
        started.append(copy)
        return copy

    first, own_far, second = {}, {}, {}

    def send_own(m):
        a, b = piece(wide, m, me, 0), piece(wide, m, me, 1)
        first[m] = (
            [begin(remote(a, a, dp_peer(my, x_at(d)))) for d in range(1, gx)],
            [begin(remote(b, b, dp_peer(y_at(d), mx))) for d in range(1, gy)],
        )
        own_far[m] = [begin(remote(a, a, dp_peer(y_at(d), mx))) for d in range(1, gy)] + [
            begin(remote(b, b, dp_peer(my, x_at(d)))) for d in range(1, gx)
        ]

    def forward(m):
        second[m] = []
        for d in range(1, gx):
            first[m][0][d - 1].wait_recv()
            a = piece(wide, m, my * gx + x_at(gx - d), 0)
            for e in range(1, gy):
                second[m].append(begin(remote(a, a, dp_peer(y_at(e), mx))))
        for d in range(1, gy):
            first[m][1][d - 1].wait_recv()
            b = piece(wide, m, y_at(gy - d) * gx + mx, 1)
            for e in range(1, gx):
                second[m].append(begin(remote(b, b, dp_peer(my, x_at(e)))))

    def gathered(m):
        for copy in own_far[m] + second[m]:
            copy.wait_recv()

    send_own(0)
    send_own(1)
    ups = [remote(near.at[m], before.at[m], (lax.rem(ci + 1, c), me)) for m in range(3)]
    downs = [remote(near.at[m], after.at[m], (lax.rem(ci + c - 1, c), me)) for m in range(3)]
    has_next, has_prev = ci < c - 1, ci > 0

    @pl.when(has_next)
    def _():
        for copy in ups:
            copy.start()

    @pl.when(has_prev)
    def _():
        for copy in downs:
            copy.start()

    send_own(2)

    row_of = jnp.broadcast_to(picks[...], (LANES, batch)).T
    lab_t[...] = jnp.broadcast_to(labs[...], (LANES, batch)).T
    lane = lax.broadcasted_iota(jnp.int32, (batch, LANES), 1)
    for k in range(pool_v.shape[0] // LANES):
        hot[:, k * LANES : (k + 1) * LANES] = (row_of == lane + k * LANES).astype(F32).astype(BF16)
    loads[3].wait()

    def column(t):
        return pl.ds(pl.multiple_of(t * TILE, TILE), TILE)

    @pl.loop(0, tiles)
    def _(t):
        at = column(t)
        rows[:, at] = dot_nn(hot[...], pool_v[:, at]).astype(BF16)

    forward(0)

    for load in loads[4:]:
        load.wait()
    widened(edge.at[2], 1)

    @pl.when(has_prev)
    def _():
        for copy in ups:
            copy.wait_recv()

    @pl.when(has_next)
    def _():
        for copy in downs:
            copy.wait_recv()

    def differences(m, at):
        mine = own[m, at, :]
        fixed = edge[m, at, :]
        left = jnp.where(ci == 0, fixed, before[m, at, :].astype(F32))
        right = jnp.where(ci == c - 1, fixed, after[m, at, :].astype(F32))
        return right - mine, mine - left

    zero = jnp.zeros((8, LANES), F32)

    def span_sums(m, carry):
        def body(r, carry):
            ahead, behind = differences(m, pl.ds(pl.multiple_of(r * step, step), step))
            return (
                carry[0] + fold(ahead * ahead),
                carry[1] + fold(behind * behind),
                carry[2] + fold(ahead * behind),
            )

        return lax.fori_loop(0, block // step, body, carry)

    carry = (zero, zero, zero)
    for m in range(3):
        carry = span_sums(m, carry)
    for k in range(3):
        sums[me, k] = carry[k]
    sums_out = [
        begin(remote(sums.at[me], sums.at[me], (ci, lax.rem(me + d, n)))) for d in range(1, n)
    ]

    forward(1)
    gathered(0)

    @pl.loop(0, tiles)
    def _(t):
        at = column(t)
        pre = dot_nn(rows[...], wide[0, :, at])
        sig = jax.nn.sigmoid(pre)
        hid[:, at] = (pre * sig).astype(BF16)
        slope[:, at] = sig * (1.0 + pre * (1.0 - sig))

    forward(2)

    for copy in sums_out:
        copy.wait_recv()

    def over_dp(ref, k):
        total = ref[0, k]
        for j in range(1, n):
            total = total + ref[j, k]
        return whole(total)

    sq_ahead, sq_behind, cross = (over_dp(sums, k) for k in range(3))
    len_ahead = jnp.sqrt(sq_ahead + EPS)
    len_behind = jnp.sqrt(sq_behind + EPS)
    raw_sq = (
        sq_ahead / (len_ahead * len_ahead)
        + sq_behind / (len_behind * len_behind)
        + 2.0 * cross / (len_ahead * len_behind)
    )
    raw_len = jnp.sqrt(raw_sq + EPS)
    spans[ci, 0] = jnp.broadcast_to(len_behind, (8, LANES))
    spans[ci, 1] = jnp.broadcast_to(len_ahead, (8, LANES))
    spans_out = [
        begin(remote(spans.at[ci], spans.at[ci], (lax.rem(ci + d, c), me))) for d in range(1, c)
    ]

    gathered(1)

    @pl.loop(0, tiles)
    def _(t):
        at = column(t)
        resid[:, at] = (rows[:, at].astype(F32) + dot_nn(hid[...], wide[1, :, at])).astype(BF16)

    gathered(2)

    def classify(t, energy):
        at = column(t)
        logits = dot_nn(resid[...], wide[2, :, at])
        parts = []
        for k in range(TILE // LANES):
            target = (lab_t[...] == lane + (t * TILE + k * LANES)).astype(F32)
            err = logits[:, k * LANES : (k + 1) * LANES] - target
            energy = energy + fold(err * err)
            parts.append((err * norm).astype(BF16))
        dlog[:, at] = jnp.concatenate(parts, axis=1)
        return energy

    energy = lax.fori_loop(0, tiles, classify, zero)

    def products(m, left, right):
        @pl.loop(0, depth // TILE)
        def _(t):
            at = column(t)
            grad[m, at, :] = dot_tn(left[:, at], right[...]).astype(BF16)

    to_rows, to_cols, back_x, back_y = {}, {}, {}, {}

    def scatter(m):
        to_rows[m], to_cols[m] = [], []
        for d in range(1, gy):
            for x in range(gx):
                to_rows[m].append(
                    begin(
                        remote(
                            piece(grad, m, y_at(d) * gx + x, 0),
                            from_y.at[m, d - 1, x],
                            dp_peer(y_at(d), mx),
                        )
                    )
                )
        for d in range(1, gx):
            for y in range(gy):
                to_cols[m].append(
                    begin(
                        remote(
                            piece(grad, m, y * gx + x_at(d), 1),
                            from_x.at[m, d - 1, y],
                            dp_peer(my, x_at(d)),
                        )
                    )
                )

    def combine(m, index, h, arrived, count, slot):
        def body(r, _):
            off = pl.multiple_of(r * step, step)
            at = pl.ds(pl.multiple_of(index * block + h * half + off, step), step)
            total = grad[m, at, :].astype(F32)
            for d in range(count):
                total = total + arrived[m, d, slot, pl.ds(off, step), :].astype(F32)
            grad[m, at, :] = total.astype(BF16)
            return 0

        lax.fori_loop(0, half // step, body, 0)

    def scatter_on(m):
        for copy in to_rows[m]:
            copy.wait_recv()
        back_x[m] = []
        for d in range(1, gx):
            index = my * gx + x_at(d)
            combine(m, index, 0, from_y, gy - 1, x_at(d))
            back_x[m].append(
                begin(remote(piece(grad, m, index, 0), last_x.at[m, d - 1], dp_peer(my, x_at(d))))
            )
        for copy in to_cols[m]:
            copy.wait_recv()
        back_y[m] = []
        for d in range(1, gy):
            index = y_at(d) * gx + mx
            combine(m, index, 1, from_x, gx - 1, y_at(d))
            back_y[m].append(
                begin(remote(piece(grad, m, index, 1), last_y.at[m, d - 1], dp_peer(y_at(d), mx)))
            )

    products(2, resid, dlog)
    scatter(2)

    @pl.loop(0, depth // TILE)
    def _(t):
        at = column(t)
        dres[:, at] = dot_nt(dlog[...], wide[2, at, :]).astype(BF16)

    products(1, hid, dres)
    scatter(1)

    @pl.loop(0, depth // TILE)
    def _(t):
        at = column(t)
        dlog[:, at] = (dot_nt(dres[...], wide[1, at, :]) * slope[:, at]).astype(BF16)

    products(0, rows, dlog)
    scatter(0)

    for copy in spans_out:
        copy.wait_recv()
    by_ahead = 1.0 / (len_ahead * raw_len)
    by_behind = 1.0 / (len_behind * raw_len)

    for m in range(3):

        def body(r, _, m=m):
            at = pl.ds(pl.multiple_of(r * step, step), step)
            ahead, behind = differences(m, at)
            tau[m, at, :] = ahead * by_ahead + behind * by_behind
            return 0

        lax.fori_loop(0, block // step, body, 0)

    arc = jnp.zeros((1, 1), F32)
    band = jnp.zeros((1, 1), F32)
    for k in range(c):
        length = spans[k, 0, 0:1, 0:1]
        arc = arc + jnp.where(k <= ci, length, 0.0)
        band = band + length
    band = band + spans[c - 1, 1, 0:1, 0:1]

    for m in (2, 1, 0):
        scatter_on(m)

    def finish(m, carry):
        for copy in back_x[m] + back_y[m]:
            copy.wait_recv()
        for h, arrived, count, slot, last, lasts in (
            (0, from_y, gy - 1, mx, last_x, gx - 1),
            (1, from_x, gx - 1, my, last_y, gy - 1),
        ):

            def body(r, carry):
                off = pl.multiple_of(r * step, step)
                total = grad[
                    m, pl.ds(pl.multiple_of(me * block + h * half + off, step), step), :
                ].astype(F32)
                for d in range(count):
                    total = total + arrived[m, d, slot, pl.ds(off, step), :].astype(F32)
                for d in range(lasts):
                    total = total + last[m, d, pl.ds(off, step), :].astype(F32)
                total = total * factor[m]
                at = pl.ds(h * half + off, step)
                edge[m, at, :] = total
                return carry[0] + fold(total * tau[m, at, :]), carry[1] + fold(total * total)

            carry = lax.fori_loop(0, half // step, body, carry)
        return carry

    carry = (zero, zero)
    for m in (2, 1, 0):
        carry = finish(m, carry)
    late[me, 0] = carry[0]
    late[me, 1] = carry[1]
    late[me, 2] = energy * (0.5 * norm)
    late_out = [
        begin(remote(late.at[me], late.at[me], (ci, lax.rem(me + d, n)))) for d in range(1, n)
    ]
    for copy in late_out:
        copy.wait_recv()
    along, g_g, energy_all = (over_dp(late, k) for k in range(3))

    goal = (ci + 1).astype(F32) / (c + 1) * band
    coef = jnp.where(climb[...] == 1, 2.0 * along, along + SPRING * (goal - arc) / band)
    tau_sq = raw_sq / (raw_sq + EPS)
    force_sq = g_g - 2.0 * coef * along + coef * coef * tau_sq
    scale = band / (c + 1) / jnp.sqrt(force_sq + EPS)
    push = scale * coef
    o_energy[...] = energy_all
    o_arc[...] = arc / band
    o_bend[...] = 0.5 * raw_len

    stores = []
    for m, out in ((2, o_out), (1, o_mid), (0, o_in)):

        def body(r, _, m=m):
            at = pl.ds(pl.multiple_of(r * step, step), step)
            new = own[m, at, :] + (push * tau[m, at, :] - scale * edge[m, at, :])
            if m == 2:
                thin[0, at, :] = new[:, :classes]
            else:
                tau[m, at, :] = new
            return 0

        lax.fori_loop(0, block // step, body, 0)
        copy = pltpu.make_async_copy(
            thin.at[0] if m == 2 else tau.at[m], out.at[0], load_sem.at[m]
        )
        copy.start()
        stores.append(copy)

    @pl.when(has_next)
    def _():
        for copy in ups:
            copy.wait_send()

    @pl.when(has_prev)
    def _():
        for copy in downs:
            copy.wait_send()

    for copy in started:
        copy.wait_send()
    for copy in stores:
        copy.wait()


def on_device(
    n,
    c,
    images_in,
    images_mid,
    images_out,
    ends_in,
    ends_mid,
    ends_out,
    data_pool,
    batch_rows,
    labels,
    climbing,
):
    block, width = images_in.shape[1], images_in.shape[2]
    classes = images_out.shape[2]
    depth = n * block
    half = block // 2
    batch = batch_rows.shape[1]
    gy, gx = grid_of(n)
    copies = copies_of(n, c)
    vmem = pl.BlockSpec(memory_space=pltpu.VMEM)
    anywhere = pl.BlockSpec(memory_space=pl.ANY)
    small = jax.ShapeDtypeStruct((1, 1), F32)
    outs = pl.pallas_call(
        functools.partial(kernel, n, c, classes),
        out_shape=(
            jax.ShapeDtypeStruct(images_in.shape, F32),
            jax.ShapeDtypeStruct(images_mid.shape, F32),
            jax.ShapeDtypeStruct(images_out.shape, F32),
            small,
            small,
            small,
        ),
        in_specs=[anywhere] * 7 + [vmem] * 3,
        out_specs=[anywhere] * 3 + [vmem] * 3,
        scratch_shapes=[
            pltpu.VMEM((3, block, width), F32),
            pltpu.VMEM((3, block, width), F32),
            pltpu.VMEM((2, block, classes), F32),
            pltpu.VMEM((3, block, width), F32),
            pltpu.VMEM((3, depth, width), BF16),
            pltpu.VMEM((3, block, width), BF16),
            pltpu.VMEM((3, block, width), BF16),
            pltpu.VMEM((3, block, width), BF16),
            pltpu.VMEM(data_pool.shape, BF16),
            pltpu.VMEM((batch, data_pool.shape[0]), BF16),
            pltpu.VMEM((batch, LANES), jnp.int32),
            pltpu.VMEM((batch, depth), BF16),
            pltpu.VMEM((batch, width), F32),
            pltpu.VMEM((batch, width), BF16),
            pltpu.VMEM((batch, depth), BF16),
            pltpu.VMEM((batch, width), BF16),
            pltpu.VMEM((batch, depth), BF16),
            pltpu.VMEM((3, depth, width), BF16),
            pltpu.VMEM((3, max(gy - 1, 1), gx, half, width), BF16),
            pltpu.VMEM((3, max(gx - 1, 1), gy, half, width), BF16),
            pltpu.VMEM((3, max(gx - 1, 1), half, width), BF16),
            pltpu.VMEM((3, max(gy - 1, 1), half, width), BF16),
            pltpu.VMEM((n, 3, 8, LANES), F32),
            pltpu.VMEM((c, 2, 8, LANES), F32),
            pltpu.VMEM((n, 3, 8, LANES), F32),
            pltpu.SemaphoreType.DMA((7,)),
            pltpu.SemaphoreType.DMA((copies,)),
            pltpu.SemaphoreType.DMA((copies,)),
        ],
        compiler_params=pltpu.CompilerParams(
            collective_id=0, has_side_effects=True, vmem_limit_bytes=63 * 1024 * 1024
        ),
    )(
        images_in,
        images_mid,
        images_out,
        ends_in,
        ends_mid,
        ends_out,
        data_pool,
        batch_rows,
        labels,
        climbing[:, None],
    )
    return (*outs[:3], outs[3][0], outs[4][0], outs[5][0])


def solution(mesh):
    placed = (
        P("chain", "dp", None),
        P("chain", "dp", None),
        P("chain", "dp", None),
        P(None, "dp", None),
        P(None, "dp", None),
        P(None, "dp", None),
        P("dp", None),
        P("chain", "dp"),
        P("chain", "dp"),
        P("chain"),
    )
    return jax.shard_map(
        functools.partial(on_device, mesh.shape["dp"], mesh.shape["chain"]),
        mesh=mesh,
        in_specs=placed,
        out_specs=(
            P("chain", "dp", None),
            P("chain", "dp", None),
            P("chain", "dp", None),
            P("chain"),
            P("chain"),
            P("chain"),
        ),
        check_vma=False,
    )
```

```python
import functools

import jax
import jax.numpy as jnp
from jax import lax
from jax.experimental import pallas as pl
from jax.experimental.pallas import tpu as pltpu
from jax.sharding import PartitionSpec as P

SPRING = 0.03
EPS = 1e-06
TILE = 256
LANES = 128
F32 = jnp.float32
BF16 = jnp.bfloat16


def grid_of(count):
    rows = max(k for k in range(1, count + 1) if count % k == 0 and k * k <= count)
    return rows, count // rows


def copies_of(count, chain, chunks):
    gy, gx = grid_of(count)
    gather = 2 * (gx - 1) + 2 * (gy - 1) + 2 * (gx - 1) * (gy - 1)
    scatter = (gy - 1) * gx + (gx - 1) * gy
    back = (gx - 1) + (gy - 1)
    return (2 + chunks) * (gather + scatter) + 3 * back + 2 * (count - 1) + (chain - 1) + 6


def dot_nn(left, right):
    return jnp.dot(left, right, preferred_element_type=F32)


def dot_nt(left, right):
    return lax.dot_general(left, right, (((1,), (1,)), ((), ())), preferred_element_type=F32)


def dot_tn(left, right):
    return lax.dot_general(left, right, (((0,), (0,)), ((), ())), preferred_element_type=F32)


def fold(value):
    part = jnp.sum(value.reshape(value.shape[0] // 8, 8, value.shape[1]), axis=0)
    total = part[:, :LANES]
    for k in range(1, value.shape[1] // LANES):
        total = total + part[:, k * LANES : (k + 1) * LANES]
    return total


def whole(tile):
    return jnp.sum(tile, axis=(0, 1), keepdims=True)


def kernel(
    n,
    c,
    classes,
    p_in,
    p_mid,
    p_out,
    e_in,
    e_mid,
    e_out,
    pool,
    picks,
    labs,
    climb,
    o_in,
    o_mid,
    o_out,
    o_energy,
    o_arc,
    o_bend,
    own,
    edge,
    thin,
    tau,
    wide,
    near,
    before,
    after,
    pool_v,
    hot,
    lab_t,
    rows,
    slope,
    hid,
    resid,
    rows_t,
    hid_t,
    resid_t,
    dlog,
    dres,
    grad,
    from_y,
    from_x,
    last_x,
    last_y,
    sums,
    spans,
    late,
    load_sem,
    send_sem,
    recv_sem,
):
    ci, me = lax.axis_index("chain"), lax.axis_index("dp")
    gy, gx = grid_of(n)
    my, mx = me // gx, lax.rem(me, gx)
    block, width = own.shape[1], own.shape[2]
    depth = n * block
    half = block // 2
    step = min(32, half)
    batch = rows.shape[0]
    tiles = width // TILE
    factor = (depth**-0.5, width**-0.5, depth**-0.5)
    norm = 1.0 / (batch * n * classes)
    counter = [0]

    def remote(src, dst, to):
        k = counter[0]
        counter[0] += 1
        copy = pltpu.make_async_remote_copy(
            src_ref=src,
            dst_ref=dst,
            send_sem=send_sem.at[k],
            recv_sem=recv_sem.at[k],
            device_id=to,
            device_id_type=pl.DeviceIdType.MESH,
        )
        return copy

    def dp_peer(y, x):
        return (ci, y * gx + x)

    def y_at(d):
        return lax.rem(my + d, gy)

    def x_at(d):
        return lax.rem(mx + d, gx)

    barrier = pltpu.get_barrier_semaphore()
    for d in range(1, n):
        pl.semaphore_signal(
            barrier, inc=1, device_id=(ci, lax.rem(me + d, n)), device_id_type=pl.DeviceIdType.MESH
        )
    for d in range(1, c):
        pl.semaphore_signal(
            barrier, inc=1, device_id=(lax.rem(ci + d, c), me), device_id_type=pl.DeviceIdType.MESH
        )

    end = jnp.where(ci == 0, 0, 1)
    loads = [
        pltpu.make_async_copy(p_in.at[0], own.at[0], load_sem.at[0]),
        pltpu.make_async_copy(p_mid.at[0], own.at[1], load_sem.at[1]),
        pltpu.make_async_copy(p_out.at[0], thin.at[0, pl.ds(0, classes)], load_sem.at[2]),
        pltpu.make_async_copy(pool, pool_v, load_sem.at[3]),
        pltpu.make_async_copy(e_in.at[end], edge.at[0], load_sem.at[4]),
        pltpu.make_async_copy(e_mid.at[end], edge.at[1], load_sem.at[5]),
        pltpu.make_async_copy(e_out.at[end], thin.at[1, pl.ds(0, classes)], load_sem.at[6]),
    ]
    for load in loads:
        load.start()

    def turned(into, thin_at):
        @pl.loop(0, width // LANES)
        def _(k):
            at = pl.ds(pl.multiple_of(k * LANES, LANES), LANES)
            into[:, at] = thin[thin_at, at, :].T

    def blanked(thin_at):
        if classes < width:
            thin[thin_at, pl.ds(classes, width - classes), :] = jnp.zeros(
                (width - classes, block), F32
            )

    def lowered(m):
        def body(r, _):
            off = pl.multiple_of(r * step, step)
            value = own[m, pl.ds(off, step), :]
            wide[m, pl.ds(pl.multiple_of(me * block + off, step), step), :] = (
                value * factor[m]
            ).astype(BF16)
            near[m, pl.ds(off, step), :] = value.astype(BF16)
            return 0

        lax.fori_loop(0, block // step, body, 0)

    for m in range(2):
        loads[m].wait()
        lowered(m)
    blanked(0)
    blanked(1)
    pl.semaphore_wait(barrier, n - 1 + c - 1)

    def column(t):
        return pl.ds(pl.multiple_of(t * TILE, TILE), TILE)

    everything = pl.ds(0, width)

    def piece(ref, m, index, h, at=everything):
        return ref.at[m, pl.ds(pl.multiple_of(index * block + h * half, half), half), at]

    started = []

    def begin(copy):
        copy.start()
        started.append(copy)
        return copy

    first, own_far, second = {}, {}, {}

    def send_own(key, m, at=everything):
        a, b = piece(wide, m, me, 0, at), piece(wide, m, me, 1, at)
        first[key] = (
            [begin(remote(a, a, dp_peer(my, x_at(d)))) for d in range(1, gx)],
            [begin(remote(b, b, dp_peer(y_at(d), mx))) for d in range(1, gy)],
        )
        own_far[key] = [begin(remote(a, a, dp_peer(y_at(d), mx))) for d in range(1, gy)] + [
            begin(remote(b, b, dp_peer(my, x_at(d)))) for d in range(1, gx)
        ]

    def forward(key, m, at=everything):
        second[key] = []
        for d in range(1, gx):
            first[key][0][d - 1].wait_recv()
            a = piece(wide, m, my * gx + x_at(gx - d), 0, at)
            for e in range(1, gy):
                second[key].append(begin(remote(a, a, dp_peer(y_at(e), mx))))
        for d in range(1, gy):
            first[key][1][d - 1].wait_recv()
            b = piece(wide, m, y_at(gy - d) * gx + mx, 1, at)
            for e in range(1, gx):
                second[key].append(begin(remote(b, b, dp_peer(my, x_at(e)))))

    def gathered(key):
        for copy in own_far[key] + second[key]:
            copy.wait_recv()

    def send_chunk(t):
        if t < tiles:
            send_own((2, t), 2, pl.ds(t * TILE, TILE))

    def forward_chunk(t):
        if t < tiles:
            forward((2, t), 2, pl.ds(t * TILE, TILE))

    send_own(0, 0)
    send_own(1, 1)
    loads[2].wait()
    turned(own.at[2], 0)
    lowered(2)
    ups = [remote(near.at[m], before.at[m], (lax.rem(ci + 1, c), me)) for m in range(3)]
    downs = [remote(near.at[m], after.at[m], (lax.rem(ci + c - 1, c), me)) for m in range(3)]
    has_next, has_prev = ci < c - 1, ci > 0

    @pl.when(has_next)
    def _():
        for copy in ups:
            copy.start()

    @pl.when(has_prev)
    def _():
        for copy in downs:
            copy.start()

    row_of = jnp.broadcast_to(picks[...], (LANES, batch)).T
    lab_t[...] = jnp.broadcast_to(labs[...], (LANES, batch)).T
    lane = lax.broadcasted_iota(jnp.int32, (batch, LANES), 1)
    for k in range(pool_v.shape[0] // LANES):
        hot[:, k * LANES : (k + 1) * LANES] = (row_of == lane + k * LANES).astype(F32).astype(BF16)
    loads[3].wait()

    @pl.loop(0, tiles)
    def _(t):
        at = column(t)
        picked = dot_nn(hot[...], pool_v[:, at]).astype(BF16)
        rows[:, at] = picked
        rows_t[at, :] = picked.T

    forward(0, 0)
    send_chunk(0)

    for load in loads[4:]:
        load.wait()
    turned(edge.at[2], 1)

    @pl.when(has_prev)
    def _():
        for copy in ups:
            copy.wait_recv()

    @pl.when(has_next)
    def _():
        for copy in downs:
            copy.wait_recv()

    def differences(m, at):
        mine = own[m, at, :]
        fixed = edge[m, at, :]
        left = jnp.where(ci == 0, fixed, before[m, at, :].astype(F32))
        right = jnp.where(ci == c - 1, fixed, after[m, at, :].astype(F32))
        return right - mine, mine - left

    zero = jnp.zeros((8, LANES), F32)

    def span_sums(m, carry):
        def body(r, carry):
            ahead, behind = differences(m, pl.ds(pl.multiple_of(r * step, step), step))
            return (
                carry[0] + fold(ahead * ahead),
                carry[1] + fold(behind * behind),
                carry[2] + fold(ahead * behind),
            )

        return lax.fori_loop(0, block // step, body, carry)

    carry = (zero, zero, zero)
    for m in range(3):
        carry = span_sums(m, carry)
    for k in range(3):
        sums[me, k] = carry[k]
    sums_out = [
        begin(remote(sums.at[me], sums.at[me], (ci, lax.rem(me + d, n)))) for d in range(1, n)
    ]

    forward(1, 1)
    send_chunk(1)
    gathered(0)

    @pl.loop(0, tiles)
    def _(t):
        at = column(t)
        pre = dot_nn(rows[...], wide[0, :, at])
        sig = jax.nn.sigmoid(pre)
        value = (pre * sig).astype(BF16)
        hid[:, at] = value
        hid_t[at, :] = value.T
        slope[:, at] = sig * (1.0 + pre * (1.0 - sig))

    forward_chunk(0)
    send_chunk(2)

    for copy in sums_out:
        copy.wait_recv()

    def over_dp(ref, k):
        total = ref[0, k]
        for j in range(1, n):
            total = total + ref[j, k]
        return whole(total)

    sq_ahead, sq_behind, cross = (over_dp(sums, k) for k in range(3))
    len_ahead = jnp.sqrt(sq_ahead + EPS)
    len_behind = jnp.sqrt(sq_behind + EPS)
    raw_sq = (
        sq_ahead / (len_ahead * len_ahead)
        + sq_behind / (len_behind * len_behind)
        + 2.0 * cross / (len_ahead * len_behind)
    )
    raw_len = jnp.sqrt(raw_sq + EPS)
    spans[ci, 0] = jnp.broadcast_to(len_behind, (8, LANES))
    spans[ci, 1] = jnp.broadcast_to(len_ahead, (8, LANES))
    spans_out = [
        begin(remote(spans.at[ci], spans.at[ci], (lax.rem(ci + d, c), me))) for d in range(1, c)
    ]

    gathered(1)

    @pl.loop(0, tiles)
    def _(t):
        at = column(t)
        value = (rows[:, at].astype(F32) + dot_nn(hid[...], wide[1, :, at])).astype(BF16)
        resid[:, at] = value
        resid_t[at, :] = value.T

    forward_chunk(1)
    send_chunk(3)

    def classify(t, energy):
        at = column(t)
        logits = dot_nn(resid[...], wide[2, :, at])
        parts = []
        for k in range(TILE // LANES):
            target = (lab_t[...] == lane + (t * TILE + k * LANES)).astype(F32)
            err = logits[:, k * LANES : (k + 1) * LANES] - target
            energy = energy + fold(err * err)
            parts.append((err * norm).astype(BF16))
        dlog[:, at] = jnp.concatenate(parts, axis=1)
        return energy

    def products(m, left_t, right):
        @pl.loop(0, depth // TILE)
        def _(t):
            at = column(t)
            grad[m, at, :] = dot_nn(left_t[at, :], right[...]).astype(BF16)

    to_rows, to_cols, back_x, back_y = {}, {}, {}, {}

    def scatter(m, at=everything):
        to_rows.setdefault(m, [])
        to_cols.setdefault(m, [])
        for d in range(1, gy):
            for x in range(gx):
                to_rows[m].append(
                    begin(
                        remote(
                            piece(grad, m, y_at(d) * gx + x, 0, at),
                            from_y.at[m, d - 1, x, :, at],
                            dp_peer(y_at(d), mx),
                        )
                    )
                )
        for d in range(1, gx):
            for y in range(gy):
                to_cols[m].append(
                    begin(
                        remote(
                            piece(grad, m, y * gx + x_at(d), 1, at),
                            from_x.at[m, d - 1, y, :, at],
                            dp_peer(my, x_at(d)),
                        )
                    )
                )

    def combine(m, index, h, arrived, count, slot):
        def body(r, _):
            off = pl.multiple_of(r * step, step)
            at = pl.ds(pl.multiple_of(index * block + h * half + off, step), step)
            total = grad[m, at, :].astype(F32)
            for d in range(count):
                total = total + arrived[m, d, slot, pl.ds(off, step), :].astype(F32)
            grad[m, at, :] = total.astype(BF16)
            return 0

        lax.fori_loop(0, half // step, body, 0)

    def scatter_on(m):
        for copy in to_rows[m]:
            copy.wait_recv()
        back_x[m] = []
        for d in range(1, gx):
            index = my * gx + x_at(d)
            combine(m, index, 0, from_y, gy - 1, x_at(d))
            back_x[m].append(
                begin(remote(piece(grad, m, index, 0), last_x.at[m, d - 1], dp_peer(my, x_at(d))))
            )
        for copy in to_cols[m]:
            copy.wait_recv()
        back_y[m] = []
        for d in range(1, gy):
            index = y_at(d) * gx + mx
            combine(m, index, 1, from_x, gx - 1, y_at(d))
            back_y[m].append(
                begin(remote(piece(grad, m, index, 1), last_y.at[m, d - 1], dp_peer(y_at(d), mx)))
            )

    energy = zero
    for t in range(tiles):
        gathered((2, t))
        energy = classify(t, energy)
        at = pl.ds(t * TILE, TILE)

        @pl.loop(0, depth // TILE)
        def _(r):
            of = column(r)
            grad[2, of, at] = dot_nn(resid_t[of, :], dlog[:, at]).astype(BF16)

        forward_chunk(t + 2)
        send_chunk(t + 4)
        scatter(2, at)

    @pl.loop(0, depth // TILE)
    def _(t):
        at = column(t)
        dres[:, at] = dot_nt(dlog[...], wide[2, at, :]).astype(BF16)

    products(1, hid_t, dres)
    scatter(1)

    @pl.loop(0, depth // TILE)
    def _(t):
        at = column(t)
        dlog[:, at] = (dot_nt(dres[...], wide[1, at, :]) * slope[:, at]).astype(BF16)

    products(0, rows_t, dlog)
    scatter(0)

    for copy in spans_out:
        copy.wait_recv()
    by_ahead = 1.0 / (len_ahead * raw_len)
    by_behind = 1.0 / (len_behind * raw_len)

    for m in range(3):

        def body(r, _, m=m):
            at = pl.ds(pl.multiple_of(r * step, step), step)
            ahead, behind = differences(m, at)
            tau[m, at, :] = ahead * by_ahead + behind * by_behind
            return 0

        lax.fori_loop(0, block // step, body, 0)

    arc = jnp.zeros((1, 1), F32)
    band = jnp.zeros((1, 1), F32)
    for k in range(c):
        length = spans[k, 0, 0:1, 0:1]
        arc = arc + jnp.where(k <= ci, length, 0.0)
        band = band + length
    band = band + spans[c - 1, 1, 0:1, 0:1]

    for m in (2, 1, 0):
        scatter_on(m)

    def finish(m, carry):
        for copy in back_x[m] + back_y[m]:
            copy.wait_recv()
        for h, arrived, count, slot, last, lasts in (
            (0, from_y, gy - 1, mx, last_x, gx - 1),
            (1, from_x, gx - 1, my, last_y, gy - 1),
        ):

            def body(r, carry):
                off = pl.multiple_of(r * step, step)
                total = grad[
                    m, pl.ds(pl.multiple_of(me * block + h * half + off, step), step), :
                ].astype(F32)
                for d in range(count):
                    total = total + arrived[m, d, slot, pl.ds(off, step), :].astype(F32)
                for d in range(lasts):
                    total = total + last[m, d, pl.ds(off, step), :].astype(F32)
                total = total * factor[m]
                at = pl.ds(h * half + off, step)
                edge[m, at, :] = total
                return carry[0] + fold(total * tau[m, at, :]), carry[1] + fold(total * total)

            carry = lax.fori_loop(0, half // step, body, carry)
        return carry

    carry = (zero, zero)
    for m in (2, 1, 0):
        carry = finish(m, carry)
    late[me, 0] = carry[0]
    late[me, 1] = carry[1]
    late[me, 2] = energy * (0.5 * norm)
    late_out = [
        begin(remote(late.at[me], late.at[me], (ci, lax.rem(me + d, n)))) for d in range(1, n)
    ]
    for copy in late_out:
        copy.wait_recv()
    along, g_g, energy_all = (over_dp(late, k) for k in range(3))

    goal = (ci + 1).astype(F32) / (c + 1) * band
    coef = jnp.where(jnp.full((1, 1), climb[0]) == 1, 2.0 * along, along + SPRING * (goal - arc) / band)
    tau_sq = raw_sq / (raw_sq + EPS)
    force_sq = g_g - 2.0 * coef * along + coef * coef * tau_sq
    scale = band / (c + 1) / jnp.sqrt(force_sq + EPS)
    push = scale * coef
    o_energy[0] = energy_all[0, 0]
    o_arc[0] = (arc / band)[0, 0]
    o_bend[0] = (0.5 * raw_len)[0, 0]

    stores = []
    for m, out in ((2, o_out), (1, o_mid), (0, o_in)):
        if m == 2:

            @pl.loop(0, width // LANES)
            def _(k):
                at = pl.ds(pl.multiple_of(k * LANES, LANES), LANES)
                new = own[2, :, at] + (push * tau[2, :, at] - scale * edge[2, :, at])
                thin[0, at, :] = new.T

            source = thin.at[0, pl.ds(0, classes)]
        else:

            @pl.loop(0, block // step)
            def _(r):
                at = pl.ds(pl.multiple_of(r * step, step), step)
                tau[m, at, :] = own[m, at, :] + (push * tau[m, at, :] - scale * edge[m, at, :])

            source = tau.at[m]
        copy = pltpu.make_async_copy(source, out.at[0], load_sem.at[m])
        copy.start()
        stores.append(copy)

    @pl.when(has_next)
    def _():
        for copy in ups:
            copy.wait_send()

    @pl.when(has_prev)
    def _():
        for copy in downs:
            copy.wait_send()

    for copy in started:
        copy.wait_send()
    for copy in stores:
        copy.wait()


def on_device(
    n,
    c,
    images_in,
    images_mid,
    images_out,
    ends_in,
    ends_mid,
    ends_out,
    data_pool,
    batch_rows,
    labels,
    climbing,
):
    block, width = images_in.shape[1], images_in.shape[2]
    classes = images_out.shape[2]
    depth = n * block
    half = block // 2
    batch = batch_rows.shape[1]
    gy, gx = grid_of(n)
    copies = copies_of(n, c, width // TILE)
    vmem = pl.BlockSpec(memory_space=pltpu.VMEM)
    anywhere = pl.BlockSpec(memory_space=pl.ANY)
    scalar = pl.BlockSpec(memory_space=pltpu.SMEM)
    small = jax.ShapeDtypeStruct((1,), F32)
    outs = pl.pallas_call(
        functools.partial(kernel, n, c, classes),
        out_shape=(
            jax.ShapeDtypeStruct(images_in.shape, F32),
            jax.ShapeDtypeStruct(images_mid.shape, F32),
            jax.ShapeDtypeStruct((1, classes, block), F32),
            small,
            small,
            small,
        ),
        in_specs=[anywhere] * 7 + [vmem] * 2 + [scalar],
        out_specs=[anywhere] * 3 + [scalar] * 3,
        scratch_shapes=[
            pltpu.VMEM((3, block, width), F32),
            pltpu.VMEM((3, block, width), F32),
            pltpu.VMEM((2, width, block), F32),
            pltpu.VMEM((3, block, width), F32),
            pltpu.VMEM((3, depth, width), BF16),
            pltpu.VMEM((3, block, width), BF16),
            pltpu.VMEM((3, block, width), BF16),
            pltpu.VMEM((3, block, width), BF16),
            pltpu.VMEM(data_pool.shape, BF16),
            pltpu.VMEM((batch, data_pool.shape[0]), BF16),
            pltpu.VMEM((batch, LANES), jnp.int32),
            pltpu.VMEM((batch, depth), BF16),
            pltpu.VMEM((batch, width), F32),
            pltpu.VMEM((batch, width), BF16),
            pltpu.VMEM((batch, depth), BF16),
            pltpu.VMEM((depth, batch), BF16),
            pltpu.VMEM((width, batch), BF16),
            pltpu.VMEM((depth, batch), BF16),
            pltpu.VMEM((batch, width), BF16),
            pltpu.VMEM((batch, depth), BF16),
            pltpu.VMEM((3, depth, width), BF16),
            pltpu.VMEM((3, max(gy - 1, 1), gx, half, width), BF16),
            pltpu.VMEM((3, max(gx - 1, 1), gy, half, width), BF16),
            pltpu.VMEM((3, max(gx - 1, 1), half, width), BF16),
            pltpu.VMEM((3, max(gy - 1, 1), half, width), BF16),
            pltpu.VMEM((n, 3, 8, LANES), F32),
            pltpu.VMEM((c, 2, 8, LANES), F32),
            pltpu.VMEM((n, 3, 8, LANES), F32),
            pltpu.SemaphoreType.DMA((7,)),
            pltpu.SemaphoreType.DMA((copies,)),
            pltpu.SemaphoreType.DMA((copies,)),
        ],
        compiler_params=pltpu.CompilerParams(
            collective_id=0, has_side_effects=True, vmem_limit_bytes=63 * 1024 * 1024
        ),
    )(
        images_in,
        images_mid,
        jnp.swapaxes(images_out, 1, 2),
        ends_in,
        ends_mid,
        jnp.swapaxes(ends_out, 1, 2),
        data_pool,
        batch_rows,
        labels,
        climbing,
    )
    return (outs[0], outs[1], jnp.swapaxes(outs[2], 1, 2), *outs[3:])


def solution(mesh):
    placed = (
        P("chain", "dp", None),
        P("chain", "dp", None),
        P("chain", "dp", None),
        P(None, "dp", None),
        P(None, "dp", None),
        P(None, "dp", None),
        P("dp", None),
        P("chain", "dp"),
        P("chain", "dp"),
        P("chain"),
    )
    return jax.shard_map(
        functools.partial(on_device, mesh.shape["dp"], mesh.shape["chain"]),
        mesh=mesh,
        in_specs=placed,
        out_specs=(
            P("chain", "dp", None),
            P("chain", "dp", None),
            P("chain", "dp", None),
            P("chain"),
            P("chain"),
            P("chain"),
        ),
        check_vma=False,
    )
```

```python
import functools

import jax
import jax.numpy as jnp
from jax import lax
from jax.experimental import pallas as pl
from jax.experimental.pallas import tpu as pltpu
from jax.sharding import PartitionSpec as P

SPRING = 0.03
EPS = 1e-06
TILE = 256
LANES = 128
F32 = jnp.float32
BF16 = jnp.bfloat16


def copies_of(count, chain, chunks):
    pairs = count // 2
    gather = 1 + (pairs - 1) + pairs
    scatter = pairs
    return (2 + chunks) * (gather + scatter) + 3 * pairs + 2 * (count - 1) + (chain - 1) + 9


def dot_nn(left, right):
    return jnp.dot(left, right, preferred_element_type=F32)


def dot_nt(left, right):
    return lax.dot_general(left, right, (((1,), (1,)), ((), ())), preferred_element_type=F32)


def dot_tn(left, right):
    return lax.dot_general(left, right, (((0,), (0,)), ((), ())), preferred_element_type=F32)


def fold(value):
    part = jnp.sum(value.reshape(value.shape[0] // 8, 8, value.shape[1]), axis=0)
    total = part[:, :LANES]
    for k in range(1, value.shape[1] // LANES):
        total = total + part[:, k * LANES : (k + 1) * LANES]
    return total


def whole(tile):
    return jnp.sum(tile, axis=(0, 1), keepdims=True)


def kernel(
    n,
    c,
    classes,
    p_in,
    p_mid,
    p_out,
    e_in,
    e_mid,
    e_out,
    pool,
    picks,
    labs,
    climb,
    o_in,
    o_mid,
    o_out,
    o_energy,
    o_arc,
    o_bend,
    own,
    edge,
    thin,
    tau,
    wide,
    stage,
    near,
    before,
    after,
    pool_v,
    hot,
    lab_t,
    lab_out,
    lab_in,
    rows_out,
    rows,
    slope,
    hid,
    resid,
    rows_t,
    hid_t,
    resid_t,
    dlog,
    dres,
    grad,
    from_core,
    from_pair,
    last,
    power,
    sums,
    spans,
    late,
    load_sem,
    send_sem,
    recv_sem,
):
    ci, me = lax.axis_index("chain"), lax.axis_index("dp")
    pairs = n // 2
    core, side = lax.rem(ci, 2), lax.rem(me, 2)
    pair = me // 2
    leads = core == side
    moves = core != side
    cross = (ci + 1 - 2 * core, me + 1 - 2 * side)
    twin = (ci + 1 - 2 * core, me)
    block, width = own.shape[1], own.shape[2]
    depth = n * block
    step = min(32, block)
    batch = rows.shape[0]
    tiles = width // TILE
    factor = (depth**-0.5, width**-0.5, depth**-0.5)
    norm = 1.0 / (batch * n * classes)
    counter = [0]

    def remote(src, dst, to):
        k = counter[0]
        counter[0] += 1
        copy = pltpu.make_async_remote_copy(
            src_ref=src,
            dst_ref=dst,
            send_sem=send_sem.at[k],
            recv_sem=recv_sem.at[k],
            device_id=to,
            device_id_type=pl.DeviceIdType.MESH,
        )
        return copy

    def pair_at(d):
        return lax.rem(pair + d, pairs)

    barrier = pltpu.get_barrier_semaphore()
    for d in range(1, n):
        pl.semaphore_signal(
            barrier, inc=1, device_id=(ci, lax.rem(me + d, n)), device_id_type=pl.DeviceIdType.MESH
        )
    for d in range(1, c):
        pl.semaphore_signal(
            barrier, inc=1, device_id=(lax.rem(ci + d, c), me), device_id_type=pl.DeviceIdType.MESH
        )

    pl.semaphore_signal(barrier, inc=1, device_id=cross, device_id_type=pl.DeviceIdType.MESH)

    end = jnp.where(ci == 0, 0, 1)
    loads = [
        pltpu.make_async_copy(p_in.at[0], own.at[0], load_sem.at[0]),
        pltpu.make_async_copy(p_mid.at[0], own.at[1], load_sem.at[1]),
        pltpu.make_async_copy(p_out.at[0], thin.at[0, pl.ds(0, classes)], load_sem.at[2]),
        pltpu.make_async_copy(pool, pool_v, load_sem.at[3]),
        pltpu.make_async_copy(e_in.at[end], edge.at[0], load_sem.at[4]),
        pltpu.make_async_copy(e_mid.at[end], edge.at[1], load_sem.at[5]),
        pltpu.make_async_copy(e_out.at[end], thin.at[1, pl.ds(0, classes)], load_sem.at[6]),
    ]
    for load in loads:
        load.start()

    def turned(into, thin_at):
        @pl.loop(0, width // LANES)
        def _(k):
            at = pl.ds(pl.multiple_of(k * LANES, LANES), LANES)
            into[:, at] = thin[thin_at, at, :].T

    def blanked(thin_at):
        if classes < width:
            thin[thin_at, pl.ds(classes, width - classes), :] = jnp.zeros(
                (width - classes, block), F32
            )

    def lowered(m):
        def body(r, _):
            off = pl.multiple_of(r * step, step)
            value = own[m, pl.ds(off, step), :]
            low = (value * factor[m]).astype(BF16)
            stage[m, pl.ds(off, step), :] = low

            @pl.when(leads)
            def _():
                wide[m, pl.ds(pl.multiple_of(me * block + off, step), step), :] = low

            near[m, pl.ds(off, step), :] = value.astype(BF16)
            return 0

        lax.fori_loop(0, block // step, body, 0)

    for m in range(2):
        loads[m].wait()
        lowered(m)
    blanked(0)
    blanked(1)
    pl.semaphore_wait(barrier, n - 1 + c - 1 + 1)

    def column(t):
        return pl.ds(pl.multiple_of(t * TILE, TILE), TILE)

    everything = pl.ds(0, width)

    def piece(ref, m, index, at=everything):
        return ref.at[m, pl.ds(pl.multiple_of(index * block, block), block), at]

    started = []

    def begin(copy):
        copy.start()
        started.append(copy)
        return copy

    hop, across, over = {}, {}, {}

    def swap(src, dst):
        copy = remote(src, dst, cross)

        @pl.when(moves)
        def _():
            copy.start()

        swapped.append(copy)
        return copy

    def arrive(copy):
        @pl.when(moves)
        def _():
            copy.wait_recv()

    swapped = []

    def send_own(key, m, at=everything):
        hop[key] = swap(stage.at[m, :, at], piece(wide, m, me, at))

    def spread(key, m, at=everything):
        arrive(hop[key])
        held = piece(wide, m, 2 * pair + core, at)
        across[key] = [
            begin(remote(held, held, (ci, 2 * pair_at(d) + side))) for d in range(1, pairs)
        ]
        over[key] = [begin(remote(held, held, twin))]

    def forward(key, m, at=everything):
        for d in range(1, pairs):
            across[key][d - 1].wait_recv()
            held = piece(wide, m, 2 * pair_at(pairs - d) + core, at)
            over[key].append(begin(remote(held, held, twin)))

    def gathered(key):
        for copy in over[key]:
            copy.wait_recv()

    def chunk(step_of, t):
        step_of((2, t), 2, pl.ds(t * TILE, TILE))

    send_own(0, 0)

    lab_rows = jnp.broadcast_to(labs[...], (8, batch))
    lab_out[...] = lab_rows

    @pl.when(leads)
    def _():
        lab_in[...] = lab_rows

    row_of = jnp.broadcast_to(picks[...], (LANES, batch)).T
    lane = lax.broadcasted_iota(jnp.int32, (batch, LANES), 1)
    for k in range(pool_v.shape[0] // LANES):
        hot[:, k * LANES : (k + 1) * LANES] = (row_of == lane + k * LANES).astype(F32).astype(BF16)
    loads[3].wait()

    @pl.loop(0, tiles)
    def _(t):
        at = column(t)
        picked = dot_nn(hot[...], pool_v[:, at]).astype(BF16)
        rows_out[:, at] = picked

        @pl.when(leads)
        def _():
            rows[:, at] = picked

    lab_swap = swap(lab_out, lab_in)
    row_swap = swap(rows_out, rows)
    send_own(1, 1)
    loads[2].wait()
    turned(own.at[2], 0)
    lowered(2)
    spread(0, 0)
    for t in range(tiles):
        chunk(send_own, t)
    ups = [remote(near.at[m], before.at[m], (lax.rem(ci + 1, c), me)) for m in range(3)]
    downs = [remote(near.at[m], after.at[m], (lax.rem(ci + c - 1, c), me)) for m in range(3)]
    has_next, has_prev = ci < c - 1, ci > 0

    @pl.when(has_next)
    def _():
        for copy in ups:
            copy.start()

    @pl.when(has_prev)
    def _():
        for copy in downs:
            copy.start()

    forward(0, 0)
    arrive(lab_swap)
    lab_t[...] = jnp.broadcast_to(lab_in[...][0:1, :], (LANES, batch)).T
    arrive(row_swap)

    @pl.loop(0, tiles)
    def _(t):
        at = column(t)
        rows_t[at, :] = rows[:, at].T

    spread(1, 1)

    for load in loads[4:]:
        load.wait()
    turned(edge.at[2], 1)

    @pl.when(has_prev)
    def _():
        for copy in ups:
            copy.wait_recv()

    @pl.when(has_next)
    def _():
        for copy in downs:
            copy.wait_recv()

    def differences(m, at):
        mine = own[m, at, :]
        fixed = edge[m, at, :]
        left = jnp.where(ci == 0, fixed, before[m, at, :].astype(F32))
        right = jnp.where(ci == c - 1, fixed, after[m, at, :].astype(F32))
        return right - mine, mine - left

    zero = jnp.zeros((8, LANES), F32)

    def span_sums(m, carry):
        def body(r, carry):
            ahead, behind = differences(m, pl.ds(pl.multiple_of(r * step, step), step))
            return (
                carry[0] + fold(ahead * ahead),
                carry[1] + fold(behind * behind),
                carry[2] + fold(ahead * behind),
            )

        return lax.fori_loop(0, block // step, body, carry)

    carry = (zero, zero, zero)
    for m in range(3):
        carry = span_sums(m, carry)
    for k in range(3):
        sums[me, k] = carry[k]
    sums_out = [
        begin(remote(sums.at[me], sums.at[me], (ci, lax.rem(me + d, n)))) for d in range(1, n)
    ]

    chunk(spread, 0)
    gathered(0)

    @pl.loop(0, tiles)
    def _(t):
        at = column(t)
        pre = dot_nn(rows[...], wide[0, :, at])
        sig = jax.nn.sigmoid(pre)
        value = (pre * sig).astype(BF16)
        hid[:, at] = value
        hid_t[at, :] = value.T
        slope[:, at] = sig * (1.0 + pre * (1.0 - sig))

    forward(1, 1)
    for t in range(1, tiles):
        chunk(spread, t)

    for copy in sums_out:
        copy.wait_recv()

    def over_dp(ref, k):
        total = ref[0, k]
        for j in range(1, n):
            total = total + ref[j, k]
        return whole(total)

    sq_ahead, sq_behind, mixed = (over_dp(sums, k) for k in range(3))
    len_ahead = jnp.sqrt(sq_ahead + EPS)
    len_behind = jnp.sqrt(sq_behind + EPS)
    raw_sq = (
        sq_ahead / (len_ahead * len_ahead)
        + sq_behind / (len_behind * len_behind)
        + 2.0 * mixed / (len_ahead * len_behind)
    )
    raw_len = jnp.sqrt(raw_sq + EPS)
    spans[ci, 0] = jnp.broadcast_to(len_behind, (8, LANES))
    spans[ci, 1] = jnp.broadcast_to(len_ahead, (8, LANES))
    spans_out = [
        begin(remote(spans.at[ci], spans.at[ci], (lax.rem(ci + d, c), me))) for d in range(1, c)
    ]

    gathered(1)

    @pl.loop(0, tiles)
    def _(t):
        at = column(t)
        value = (rows[:, at].astype(F32) + dot_nn(hid[...], wide[1, :, at])).astype(BF16)
        resid[:, at] = value
        resid_t[at, :] = value.T

    chunk(forward, 0)

    def classify(t, energy):
        at = column(t)
        logits = dot_nn(resid[...], wide[2, :, at])
        parts = []
        for k in range(TILE // LANES):
            target = (lab_t[...] == lane + (t * TILE + k * LANES)).astype(F32)
            err = logits[:, k * LANES : (k + 1) * LANES] - target
            energy = energy + fold(err * err)
            parts.append((err * norm).astype(BF16))
        dlog[:, at] = jnp.concatenate(parts, axis=1)
        return energy

    def products(m, left_t, right):
        @pl.loop(0, depth // TILE)
        def _(t):
            at = column(t)
            grad[m, at, :] = dot_nn(left_t[at, :], right[...]).astype(BF16)

    to_core, to_pair, to_home = {}, {}, {}

    def scatter(m, at=everything):
        to_core.setdefault(m, [])
        for q in range(pairs):
            to_core[m].append(
                begin(
                    remote(
                        piece(grad, m, 2 * q + 1 - core, at), from_core.at[m, q, :, at], twin
                    )
                )
            )

    def combine(m, into, index, parts):
        @pl.loop(0, block // step)
        def _(r):
            off = pl.multiple_of(r * step, step)
            at = pl.ds(pl.multiple_of(index * block + off, step), step)
            total = grad[m, at, :].astype(F32)
            for part in parts:
                total = total + part[pl.ds(off, step), :].astype(F32)
            into[pl.ds(off, step), :] = total.astype(BF16)

    def scatter_on(m):
        for copy in to_core[m]:
            copy.wait_recv()
        to_pair[m] = []
        for d in range(1, pairs):
            q = pair_at(d)
            held = piece(grad, m, 2 * q + core)
            combine(m, held, 2 * q + core, [from_core.at[m, q]])
            to_pair[m].append(begin(remote(held, from_pair.at[m, d - 1], (ci, 2 * q + side))))

    def scatter_home(m):
        for copy in to_pair[m]:
            copy.wait_recv()
        parts = [from_core.at[m, pair]] + [from_pair.at[m, d] for d in range(pairs - 1)]
        held = piece(grad, m, 2 * pair + core)
        combine(m, held, 2 * pair + core, parts)

        @pl.when(leads)
        def _():
            @pl.loop(0, block // step)
            def _(r):
                off = pl.multiple_of(r * step, step)
                at = pl.ds(pl.multiple_of(me * block + off, step), step)
                last[m, pl.ds(off, step), :] = grad[m, at, :]

        to_home[m] = swap(held, last.at[m])

    energy = zero
    for t in range(tiles):
        if t + 1 < tiles:
            chunk(forward, t + 1)
        gathered((2, t))
        energy = classify(t, energy)
        at = pl.ds(t * TILE, TILE)

        @pl.loop(0, depth // TILE)
        def _(r):
            of = column(r)
            grad[2, of, at] = dot_nn(resid_t[of, :], dlog[:, at]).astype(BF16)

        scatter(2, at)

    @pl.loop(0, depth // TILE)
    def _(t):
        at = column(t)
        dres[:, at] = dot_nt(dlog[...], wide[2, at, :]).astype(BF16)

    products(1, hid_t, dres)
    scatter(1)
    scatter_on(2)

    @pl.loop(0, depth // TILE)
    def _(t):
        at = column(t)
        dlog[:, at] = (dot_nt(dres[...], wide[1, at, :]) * slope[:, at]).astype(BF16)

    products(0, rows_t, dlog)
    scatter(0)
    scatter_on(1)
    power[0] = energy * (0.5 * norm)
    power_swap = swap(power.at[0], power.at[1])

    for copy in spans_out:
        copy.wait_recv()
    by_ahead = 1.0 / (len_ahead * raw_len)
    by_behind = 1.0 / (len_behind * raw_len)

    for m in range(3):

        def body(r, _, m=m):
            at = pl.ds(pl.multiple_of(r * step, step), step)
            ahead, behind = differences(m, at)
            tau[m, at, :] = ahead * by_ahead + behind * by_behind
            return 0

        lax.fori_loop(0, block // step, body, 0)

    arc = jnp.zeros((1, 1), F32)
    band = jnp.zeros((1, 1), F32)
    for k in range(c):
        length = spans[k, 0, 0:1, 0:1]
        arc = arc + jnp.where(k <= ci, length, 0.0)
        band = band + length
    band = band + spans[c - 1, 1, 0:1, 0:1]

    scatter_on(0)
    for m in (2, 1, 0):
        scatter_home(m)
    arrive(power_swap)

    def finish(m, carry):
        arrive(to_home[m])

        def body(r, carry):
            at = pl.ds(pl.multiple_of(r * step, step), step)
            total = last[m, at, :].astype(F32) * factor[m]
            edge[m, at, :] = total
            return carry[0] + fold(total * tau[m, at, :]), carry[1] + fold(total * total)

        return lax.fori_loop(0, block // step, body, carry)

    carry = (zero, zero)
    for m in (2, 1, 0):
        carry = finish(m, carry)
    late[me, 0] = carry[0]
    late[me, 1] = carry[1]
    late[me, 2] = jnp.where(leads, power[0], power[1])
    late_out = [
        begin(remote(late.at[me], late.at[me], (ci, lax.rem(me + d, n)))) for d in range(1, n)
    ]
    for copy in late_out:
        copy.wait_recv()
    along, g_g, energy_all = (over_dp(late, k) for k in range(3))

    goal = (ci + 1).astype(F32) / (c + 1) * band
    coef = jnp.where(jnp.full((1, 1), climb[0]) == 1, 2.0 * along, along + SPRING * (goal - arc) / band)
    tau_sq = raw_sq / (raw_sq + EPS)
    force_sq = g_g - 2.0 * coef * along + coef * coef * tau_sq
    scale = band / (c + 1) / jnp.sqrt(force_sq + EPS)
    push = scale * coef
    o_energy[0] = energy_all[0, 0]
    o_arc[0] = (arc / band)[0, 0]
    o_bend[0] = (0.5 * raw_len)[0, 0]

    stores = []
    for m, out in ((2, o_out), (1, o_mid), (0, o_in)):
        if m == 2:

            @pl.loop(0, width // LANES)
            def _(k):
                at = pl.ds(pl.multiple_of(k * LANES, LANES), LANES)
                new = own[2, :, at] + (push * tau[2, :, at] - scale * edge[2, :, at])
                thin[0, at, :] = new.T

            source = thin.at[0, pl.ds(0, classes)]
        else:

            @pl.loop(0, block // step)
            def _(r):
                at = pl.ds(pl.multiple_of(r * step, step), step)
                tau[m, at, :] = own[m, at, :] + (push * tau[m, at, :] - scale * edge[m, at, :])

            source = tau.at[m]
        copy = pltpu.make_async_copy(source, out.at[0], load_sem.at[m])
        copy.start()
        stores.append(copy)

    @pl.when(has_next)
    def _():
        for copy in ups:
            copy.wait_send()

    @pl.when(has_prev)
    def _():
        for copy in downs:
            copy.wait_send()

    @pl.when(moves)
    def _():
        for copy in swapped:
            copy.wait_send()

    for copy in started:
        copy.wait_send()
    for copy in stores:
        copy.wait()


def on_device(
    n,
    c,
    images_in,
    images_mid,
    images_out,
    ends_in,
    ends_mid,
    ends_out,
    data_pool,
    batch_rows,
    labels,
    climbing,
):
    block, width = images_in.shape[1], images_in.shape[2]
    classes = images_out.shape[2]
    depth = n * block
    batch = batch_rows.shape[1]
    pairs = n // 2
    copies = copies_of(n, c, width // TILE)
    vmem = pl.BlockSpec(memory_space=pltpu.VMEM)
    anywhere = pl.BlockSpec(memory_space=pl.ANY)
    scalar = pl.BlockSpec(memory_space=pltpu.SMEM)
    small = jax.ShapeDtypeStruct((1,), F32)
    outs = pl.pallas_call(
        functools.partial(kernel, n, c, classes),
        out_shape=(
            jax.ShapeDtypeStruct(images_in.shape, F32),
            jax.ShapeDtypeStruct(images_mid.shape, F32),
            jax.ShapeDtypeStruct((1, classes, block), F32),
            small,
            small,
            small,
        ),
        in_specs=[anywhere] * 7 + [vmem] * 2 + [scalar],
        out_specs=[anywhere] * 3 + [scalar] * 3,
        scratch_shapes=[
            pltpu.VMEM((3, block, width), F32),
            pltpu.VMEM((3, block, width), F32),
            pltpu.VMEM((2, width, block), F32),
            pltpu.VMEM((3, block, width), F32),
            pltpu.VMEM((3, depth, width), BF16),
            pltpu.VMEM((3, block, width), BF16),
            pltpu.VMEM((3, block, width), BF16),
            pltpu.VMEM((3, block, width), BF16),
            pltpu.VMEM((3, block, width), BF16),
            pltpu.VMEM(data_pool.shape, BF16),
            pltpu.VMEM((batch, data_pool.shape[0]), BF16),
            pltpu.VMEM((batch, LANES), jnp.int32),
            pltpu.VMEM((8, batch), jnp.int32),
            pltpu.VMEM((8, batch), jnp.int32),
            pltpu.VMEM((batch, depth), BF16),
            pltpu.VMEM((batch, depth), BF16),
            pltpu.VMEM((batch, width), F32),
            pltpu.VMEM((batch, width), BF16),
            pltpu.VMEM((batch, depth), BF16),
            pltpu.VMEM((depth, batch), BF16),
            pltpu.VMEM((width, batch), BF16),
            pltpu.VMEM((depth, batch), BF16),
            pltpu.VMEM((batch, width), BF16),
            pltpu.VMEM((batch, depth), BF16),
            pltpu.VMEM((3, depth, width), BF16),
            pltpu.VMEM((3, pairs, block, width), BF16),
            pltpu.VMEM((3, max(pairs - 1, 1), block, width), BF16),
            pltpu.VMEM((3, block, width), BF16),
            pltpu.VMEM((2, 8, LANES), F32),
            pltpu.VMEM((n, 3, 8, LANES), F32),
            pltpu.VMEM((c, 2, 8, LANES), F32),
            pltpu.VMEM((n, 3, 8, LANES), F32),
            pltpu.SemaphoreType.DMA((7,)),
            pltpu.SemaphoreType.DMA((copies,)),
            pltpu.SemaphoreType.DMA((copies,)),
        ],
        compiler_params=pltpu.CompilerParams(
            collective_id=0, has_side_effects=True, vmem_limit_bytes=63 * 1024 * 1024
        ),
    )(
        images_in,
        images_mid,
        jnp.swapaxes(images_out, 1, 2),
        ends_in,
        ends_mid,
        jnp.swapaxes(ends_out, 1, 2),
        data_pool,
        batch_rows,
        labels,
        climbing,
    )
    return (outs[0], outs[1], jnp.swapaxes(outs[2], 1, 2), *outs[3:])


def solution(mesh):
    placed = (
        P("chain", "dp", None),
        P("chain", "dp", None),
        P("chain", "dp", None),
        P(None, "dp", None),
        P(None, "dp", None),
        P(None, "dp", None),
        P("dp", None),
        P("chain", "dp"),
        P("chain", "dp"),
        P("chain"),
    )
    return jax.shard_map(
        functools.partial(on_device, mesh.shape["dp"], mesh.shape["chain"]),
        mesh=mesh,
        in_specs=placed,
        out_specs=(
            P("chain", "dp", None),
            P("chain", "dp", None),
            P("chain", "dp", None),
            P("chain"),
            P("chain"),
            P("chain"),
        ),
        check_vma=False,
    )
```

```python
import functools

import jax
import jax.numpy as jnp
from jax import lax
from jax.experimental import pallas as pl
from jax.experimental.pallas import tpu as pltpu
from jax.sharding import PartitionSpec as P

SPRING = 0.03
EPS = 1e-06
TILE = 256
LANES = 128
F32 = jnp.float32
BF16 = jnp.bfloat16


def copies_of(count, chain, chunks):
    pairs = count // 2
    gather = 1 + (pairs - 1) + pairs
    scatter = pairs
    return (2 + chunks) * (gather + scatter + pairs) + 3 + 2 * (count - 1) + (chain - 1) + 9


def dot_nn(left, right):
    return jnp.dot(left, right, preferred_element_type=F32)


def dot_nt(left, right):
    return lax.dot_general(left, right, (((1,), (1,)), ((), ())), preferred_element_type=F32)


def dot_tn(left, right):
    return lax.dot_general(left, right, (((0,), (0,)), ((), ())), preferred_element_type=F32)


def fold(value):
    part = jnp.sum(value.reshape(value.shape[0] // 8, 8, value.shape[1]), axis=0)
    total = part[:, :LANES]
    for k in range(1, value.shape[1] // LANES):
        total = total + part[:, k * LANES : (k + 1) * LANES]
    return total


def whole(tile):
    return jnp.sum(tile, axis=(0, 1), keepdims=True)


def kernel(
    n,
    c,
    classes,
    p_in,
    p_mid,
    p_out,
    e_in,
    e_mid,
    e_out,
    pool,
    picks,
    labs,
    climb,
    o_in,
    o_mid,
    o_out,
    o_energy,
    o_arc,
    o_bend,
    own,
    edge,
    thin,
    tau,
    wide,
    stage,
    near,
    before,
    after,
    pool_v,
    hot,
    lab_t,
    lab_out,
    lab_in,
    rows_out,
    rows,
    slope,
    hid,
    resid,
    rows_t,
    hid_t,
    resid_t,
    dlog,
    dres,
    grad,
    from_core,
    from_pair,
    last,
    power,
    sums,
    spans,
    late,
    load_sem,
    send_sem,
    recv_sem,
):
    ci, me = lax.axis_index("chain"), lax.axis_index("dp")
    pairs = n // 2
    core, side = lax.rem(ci, 2), lax.rem(me, 2)
    pair = me // 2
    leads = core == side
    moves = core != side
    cross = (ci + 1 - 2 * core, me + 1 - 2 * side)
    twin = (ci + 1 - 2 * core, me)
    block, width = own.shape[1], own.shape[2]
    depth = n * block
    step = min(32, block)
    batch = rows.shape[0]
    tiles = width // TILE
    factor = (depth**-0.5, width**-0.5, depth**-0.5)
    norm = 1.0 / (batch * n * classes)
    counter = [0]

    def remote(src, dst, to):
        k = counter[0]
        counter[0] += 1
        copy = pltpu.make_async_remote_copy(
            src_ref=src,
            dst_ref=dst,
            send_sem=send_sem.at[k],
            recv_sem=recv_sem.at[k],
            device_id=to,
            device_id_type=pl.DeviceIdType.MESH,
        )
        return copy

    def pair_at(d):
        return lax.rem(pair + d, pairs)

    barrier = pltpu.get_barrier_semaphore()
    for d in range(1, n):
        pl.semaphore_signal(
            barrier, inc=1, device_id=(ci, lax.rem(me + d, n)), device_id_type=pl.DeviceIdType.MESH
        )
    for d in range(1, c):
        pl.semaphore_signal(
            barrier, inc=1, device_id=(lax.rem(ci + d, c), me), device_id_type=pl.DeviceIdType.MESH
        )

    pl.semaphore_signal(barrier, inc=1, device_id=cross, device_id_type=pl.DeviceIdType.MESH)

    end = jnp.where(ci == 0, 0, 1)
    loads = [
        pltpu.make_async_copy(p_in.at[0], own.at[0], load_sem.at[0]),
        pltpu.make_async_copy(p_mid.at[0], own.at[1], load_sem.at[1]),
        pltpu.make_async_copy(p_out.at[0], thin.at[0, pl.ds(0, classes)], load_sem.at[2]),
        pltpu.make_async_copy(pool, pool_v, load_sem.at[3]),
        pltpu.make_async_copy(e_in.at[end], edge.at[0], load_sem.at[4]),
        pltpu.make_async_copy(e_mid.at[end], edge.at[1], load_sem.at[5]),
        pltpu.make_async_copy(e_out.at[end], thin.at[1, pl.ds(0, classes)], load_sem.at[6]),
    ]
    for load in loads:
        load.start()

    def turned(into, thin_at):
        @pl.loop(0, width // LANES)
        def _(k):
            at = pl.ds(pl.multiple_of(k * LANES, LANES), LANES)
            into[:, at] = thin[thin_at, at, :].T

    def blanked(thin_at):
        if classes < width:
            thin[thin_at, pl.ds(classes, width - classes), :] = jnp.zeros(
                (width - classes, block), F32
            )

    def lowered(m):
        def body(r, _):
            off = pl.multiple_of(r * step, step)
            value = own[m, pl.ds(off, step), :]
            low = (value * factor[m]).astype(BF16)
            stage[m, pl.ds(off, step), :] = low

            @pl.when(leads)
            def _():
                wide[m, pl.ds(pl.multiple_of(me * block + off, step), step), :] = low

            near[m, pl.ds(off, step), :] = value.astype(BF16)
            return 0

        lax.fori_loop(0, block // step, body, 0)

    for m in range(2):
        loads[m].wait()
        lowered(m)
    blanked(0)
    blanked(1)
    pl.semaphore_wait(barrier, n - 1 + c - 1 + 1)

    def column(t):
        return pl.ds(pl.multiple_of(t * TILE, TILE), TILE)

    everything = pl.ds(0, width)

    def piece(ref, m, index, at=everything):
        return ref.at[m, pl.ds(pl.multiple_of(index * block, block), block), at]

    started = []

    def begin(copy):
        copy.start()
        started.append(copy)
        return copy

    hop, across, over = {}, {}, {}

    def swap(src, dst):
        copy = remote(src, dst, cross)

        @pl.when(moves)
        def _():
            copy.start()

        swapped.append(copy)
        return copy

    def arrive(copy):
        @pl.when(moves)
        def _():
            copy.wait_recv()

    swapped = []

    def send_own(key, m, at=everything):
        hop[key] = swap(stage.at[m, :, at], piece(wide, m, me, at))

    def spread(key, m, at=everything):
        arrive(hop[key])
        held = piece(wide, m, 2 * pair + core, at)
        across[key] = [
            begin(remote(held, held, (ci, 2 * pair_at(d) + side))) for d in range(1, pairs)
        ]
        over[key] = [begin(remote(held, held, twin))]

    def forward(key, m, at=everything):
        for d in range(1, pairs):
            across[key][d - 1].wait_recv()
            held = piece(wide, m, 2 * pair_at(pairs - d) + core, at)
            over[key].append(begin(remote(held, held, twin)))

    def gathered(key):
        for copy in over[key]:
            copy.wait_recv()

    def chunk(step_of, t):
        step_of((2, t), 2, pl.ds(t * TILE, TILE))

    send_own(0, 0)

    lab_rows = jnp.broadcast_to(labs[...], (8, batch))
    lab_out[...] = lab_rows

    @pl.when(leads)
    def _():
        lab_in[...] = lab_rows

    row_of = jnp.broadcast_to(picks[...], (LANES, batch)).T
    lane = lax.broadcasted_iota(jnp.int32, (batch, LANES), 1)
    for k in range(pool_v.shape[0] // LANES):
        hot[:, k * LANES : (k + 1) * LANES] = (row_of == lane + k * LANES).astype(F32).astype(BF16)
    loads[3].wait()

    @pl.loop(0, tiles)
    def _(t):
        at = column(t)
        picked = dot_nn(hot[...], pool_v[:, at]).astype(BF16)
        rows_out[:, at] = picked

        @pl.when(leads)
        def _():
            rows[:, at] = picked

    lab_swap = swap(lab_out, lab_in)
    row_swap = swap(rows_out, rows)
    send_own(1, 1)
    loads[2].wait()
    turned(own.at[2], 0)
    lowered(2)
    spread(0, 0)
    for t in range(tiles):
        chunk(send_own, t)
    ups = [remote(near.at[m], before.at[m], (lax.rem(ci + 1, c), me)) for m in range(3)]
    downs = [remote(near.at[m], after.at[m], (lax.rem(ci + c - 1, c), me)) for m in range(3)]
    has_next, has_prev = ci < c - 1, ci > 0

    @pl.when(has_next)
    def _():
        for copy in ups:
            copy.start()

    @pl.when(has_prev)
    def _():
        for copy in downs:
            copy.start()

    forward(0, 0)
    for load in loads[4:]:
        load.wait()
    turned(edge.at[2], 1)

    @pl.when(has_prev)
    def _():
        for copy in ups:
            copy.wait_recv()

    @pl.when(has_next)
    def _():
        for copy in downs:
            copy.wait_recv()

    def differences(m, at):
        mine = own[m, at, :]
        fixed = edge[m, at, :]
        left = jnp.where(ci == 0, fixed, before[m, at, :].astype(F32))
        right = jnp.where(ci == c - 1, fixed, after[m, at, :].astype(F32))
        return right - mine, mine - left

    zero = jnp.zeros((8, LANES), F32)

    def span_sums(m, carry):
        def body(r, carry):
            ahead, behind = differences(m, pl.ds(pl.multiple_of(r * step, step), step))
            return (
                carry[0] + fold(ahead * ahead),
                carry[1] + fold(behind * behind),
                carry[2] + fold(ahead * behind),
            )

        return lax.fori_loop(0, block // step, body, carry)

    carry = (zero, zero, zero)
    for m in range(3):
        carry = span_sums(m, carry)
    for k in range(3):
        sums[me, k] = carry[k]
    sums_out = [
        begin(remote(sums.at[me], sums.at[me], (ci, lax.rem(me + d, n)))) for d in range(1, n)
    ]

    arrive(lab_swap)
    lab_t[...] = jnp.broadcast_to(lab_in[...][0:1, :], (LANES, batch)).T
    arrive(row_swap)

    @pl.loop(0, tiles)
    def _(t):
        at = column(t)
        rows_t[at, :] = rows[:, at].T

    gathered(0)

    @pl.loop(0, tiles)
    def _(t):
        at = column(t)
        pre = dot_nn(rows[...], wide[0, :, at])
        sig = jax.nn.sigmoid(pre)
        value = (pre * sig).astype(BF16)
        hid[:, at] = value
        hid_t[at, :] = value.T
        slope[:, at] = sig * (1.0 + pre * (1.0 - sig))

    spread(1, 1)
    chunk(spread, 0)
    forward(1, 1)
    for t in range(1, tiles):
        chunk(spread, t)

    for copy in sums_out:
        copy.wait_recv()

    def over_dp(ref, k):
        total = ref[0, k]
        for j in range(1, n):
            total = total + ref[j, k]
        return whole(total)

    sq_ahead, sq_behind, mixed = (over_dp(sums, k) for k in range(3))
    len_ahead = jnp.sqrt(sq_ahead + EPS)
    len_behind = jnp.sqrt(sq_behind + EPS)
    raw_sq = (
        sq_ahead / (len_ahead * len_ahead)
        + sq_behind / (len_behind * len_behind)
        + 2.0 * mixed / (len_ahead * len_behind)
    )
    raw_len = jnp.sqrt(raw_sq + EPS)
    spans[ci, 0] = jnp.broadcast_to(len_behind, (8, LANES))
    spans[ci, 1] = jnp.broadcast_to(len_ahead, (8, LANES))
    spans_out = [
        begin(remote(spans.at[ci], spans.at[ci], (lax.rem(ci + d, c), me))) for d in range(1, c)
    ]

    gathered(1)

    @pl.loop(0, tiles)
    def _(t):
        at = column(t)
        value = (rows[:, at].astype(F32) + dot_nn(hid[...], wide[1, :, at])).astype(BF16)
        resid[:, at] = value
        resid_t[at, :] = value.T

    chunk(forward, 0)

    def classify(t, energy):
        at = column(t)
        logits = dot_nn(resid[...], wide[2, :, at])
        parts = []
        for k in range(TILE // LANES):
            target = (lab_t[...] == lane + (t * TILE + k * LANES)).astype(F32)
            err = logits[:, k * LANES : (k + 1) * LANES] - target
            energy = energy + fold(err * err)
            parts.append((err * norm).astype(BF16))
        dlog[:, at] = jnp.concatenate(parts, axis=1)
        return energy

    def products(m, left_t, right):
        @pl.loop(0, depth // TILE)
        def _(t):
            at = column(t)
            grad[m, at, :] = dot_nn(left_t[at, :], right[...]).astype(BF16)

    to_core, to_pair, to_home = {}, {}, {}

    def scatter(key, m, at=everything):
        to_core[key] = [
            begin(remote(piece(grad, m, 2 * q + 1 - core, at), from_core.at[m, q, :, at], twin))
            for q in range(pairs)
        ]

    def combine(m, into, index, parts, cols=everything):
        @pl.loop(0, block // step)
        def _(r):
            off = pl.multiple_of(r * step, step)
            at = pl.ds(pl.multiple_of(index * block + off, step), step)
            total = grad[m, at, cols].astype(F32)
            for part in parts:
                total = total + part[pl.ds(off, step), :].astype(F32)
            into[pl.ds(off, step), :] = total.astype(BF16)

    def scatter_on(key, m, at=everything):
        for copy in to_core[key]:
            copy.wait_recv()
        to_pair.setdefault(m, [])
        for d in range(1, pairs):
            q = pair_at(d)
            held = piece(grad, m, 2 * q + core, at)
            combine(m, held, 2 * q + core, [from_core.at[m, q, :, at]], at)
            to_pair[m].append(
                begin(remote(held, from_pair.at[m, d - 1, :, at], (ci, 2 * q + side)))
            )

    def scatter_home(m):
        for copy in to_pair[m]:
            copy.wait_recv()
        parts = [from_core.at[m, pair]] + [from_pair.at[m, d] for d in range(pairs - 1)]
        held = piece(grad, m, 2 * pair + core)
        combine(m, held, 2 * pair + core, parts)

        @pl.when(leads)
        def _():
            @pl.loop(0, block // step)
            def _(r):
                off = pl.multiple_of(r * step, step)
                at = pl.ds(pl.multiple_of(me * block + off, step), step)
                last[m, pl.ds(off, step), :] = grad[m, at, :]

        to_home[m] = swap(held, last.at[m])

    energy = zero
    for t in range(tiles):
        if t + 1 < tiles:
            chunk(forward, t + 1)
        gathered((2, t))
        energy = classify(t, energy)
        at = pl.ds(t * TILE, TILE)

        @pl.loop(0, depth // TILE)
        def _(r):
            of = column(r)
            grad[2, of, at] = dot_nn(resid_t[of, :], dlog[:, at]).astype(BF16)

        scatter((2, t), 2, at)
        if t > 0:
            chunk(scatter_on, t - 1)

    @pl.loop(0, depth // TILE)
    def _(t):
        at = column(t)
        dres[:, at] = dot_nt(dlog[...], wide[2, at, :]).astype(BF16)

    chunk(scatter_on, tiles - 1)

    products(1, hid_t, dres)
    scatter(1, 1)

    @pl.loop(0, depth // TILE)
    def _(t):
        at = column(t)
        dlog[:, at] = (dot_nt(dres[...], wide[1, at, :]) * slope[:, at]).astype(BF16)

    scatter_on(1, 1)
    products(0, rows_t, dlog)
    scatter(0, 0)
    power[0] = energy * (0.5 * norm)
    power_swap = swap(power.at[0], power.at[1])

    scatter_on(0, 0)
    scatter_home(2)

    for copy in spans_out:
        copy.wait_recv()
    by_ahead = 1.0 / (len_ahead * raw_len)
    by_behind = 1.0 / (len_behind * raw_len)

    for m in range(3):

        def body(r, _, m=m):
            at = pl.ds(pl.multiple_of(r * step, step), step)
            ahead, behind = differences(m, at)
            tau[m, at, :] = ahead * by_ahead + behind * by_behind
            return 0

        lax.fori_loop(0, block // step, body, 0)

    arc = jnp.zeros((1, 1), F32)
    band = jnp.zeros((1, 1), F32)
    for k in range(c):
        length = spans[k, 0, 0:1, 0:1]
        arc = arc + jnp.where(k <= ci, length, 0.0)
        band = band + length
    band = band + spans[c - 1, 1, 0:1, 0:1]

    for m in (1, 0):
        scatter_home(m)
    arrive(power_swap)

    def finish(m, carry):
        arrive(to_home[m])

        def body(r, carry):
            at = pl.ds(pl.multiple_of(r * step, step), step)
            total = last[m, at, :].astype(F32) * factor[m]
            edge[m, at, :] = total
            return carry[0] + fold(total * tau[m, at, :]), carry[1] + fold(total * total)

        return lax.fori_loop(0, block // step, body, carry)

    carry = (zero, zero)
    for m in (2, 1, 0):
        carry = finish(m, carry)
    late[me, 0] = carry[0]
    late[me, 1] = carry[1]
    late[me, 2] = jnp.where(leads, power[0], power[1])
    late_out = [
        begin(remote(late.at[me], late.at[me], (ci, lax.rem(me + d, n)))) for d in range(1, n)
    ]
    for copy in late_out:
        copy.wait_recv()
    along, g_g, energy_all = (over_dp(late, k) for k in range(3))

    goal = (ci + 1).astype(F32) / (c + 1) * band
    coef = jnp.where(jnp.full((1, 1), climb[0]) == 1, 2.0 * along, along + SPRING * (goal - arc) / band)
    tau_sq = raw_sq / (raw_sq + EPS)
    force_sq = g_g - 2.0 * coef * along + coef * coef * tau_sq
    scale = band / (c + 1) / jnp.sqrt(force_sq + EPS)
    push = scale * coef
    o_energy[0] = energy_all[0, 0]
    o_arc[0] = (arc / band)[0, 0]
    o_bend[0] = (0.5 * raw_len)[0, 0]

    stores = []
    for m, out in ((2, o_out), (1, o_mid), (0, o_in)):
        if m == 2:

            @pl.loop(0, width // LANES)
            def _(k):
                at = pl.ds(pl.multiple_of(k * LANES, LANES), LANES)
                new = own[2, :, at] + (push * tau[2, :, at] - scale * edge[2, :, at])
                thin[0, at, :] = new.T

            source = thin.at[0, pl.ds(0, classes)]
        else:

            @pl.loop(0, block // step)
            def _(r):
                at = pl.ds(pl.multiple_of(r * step, step), step)
                tau[m, at, :] = own[m, at, :] + (push * tau[m, at, :] - scale * edge[m, at, :])

            source = tau.at[m]
        copy = pltpu.make_async_copy(source, out.at[0], load_sem.at[m])
        copy.start()
        stores.append(copy)

    @pl.when(has_next)
    def _():
        for copy in ups:
            copy.wait_send()

    @pl.when(has_prev)
    def _():
        for copy in downs:
            copy.wait_send()

    @pl.when(moves)
    def _():
        for copy in swapped:
            copy.wait_send()

    for copy in started:
        copy.wait_send()
    for copy in stores:
        copy.wait()


def on_device(
    n,
    c,
    images_in,
    images_mid,
    images_out,
    ends_in,
    ends_mid,
    ends_out,
    data_pool,
    batch_rows,
    labels,
    climbing,
):
    block, width = images_in.shape[1], images_in.shape[2]
    classes = images_out.shape[2]
    depth = n * block
    batch = batch_rows.shape[1]
    pairs = n // 2
    copies = copies_of(n, c, width // TILE)
    vmem = pl.BlockSpec(memory_space=pltpu.VMEM)
    anywhere = pl.BlockSpec(memory_space=pl.ANY)
    scalar = pl.BlockSpec(memory_space=pltpu.SMEM)
    small = jax.ShapeDtypeStruct((1,), F32)
    outs = pl.pallas_call(
        functools.partial(kernel, n, c, classes),
        out_shape=(
            jax.ShapeDtypeStruct(images_in.shape, F32),
            jax.ShapeDtypeStruct(images_mid.shape, F32),
            jax.ShapeDtypeStruct((1, classes, block), F32),
            small,
            small,
            small,
        ),
        in_specs=[anywhere] * 7 + [vmem] * 2 + [scalar],
        out_specs=[anywhere] * 3 + [scalar] * 3,
        scratch_shapes=[
            pltpu.VMEM((3, block, width), F32),
            pltpu.VMEM((3, block, width), F32),
            pltpu.VMEM((2, width, block), F32),
            pltpu.VMEM((3, block, width), F32),
            pltpu.VMEM((3, depth, width), BF16),
            pltpu.VMEM((3, block, width), BF16),
            pltpu.VMEM((3, block, width), BF16),
            pltpu.VMEM((3, block, width), BF16),
            pltpu.VMEM((3, block, width), BF16),
            pltpu.VMEM(data_pool.shape, BF16),
            pltpu.VMEM((batch, data_pool.shape[0]), BF16),
            pltpu.VMEM((batch, LANES), jnp.int32),
            pltpu.VMEM((8, batch), jnp.int32),
            pltpu.VMEM((8, batch), jnp.int32),
            pltpu.VMEM((batch, depth), BF16),
            pltpu.VMEM((batch, depth), BF16),
            pltpu.VMEM((batch, width), F32),
            pltpu.VMEM((batch, width), BF16),
            pltpu.VMEM((batch, depth), BF16),
            pltpu.VMEM((depth, batch), BF16),
            pltpu.VMEM((width, batch), BF16),
            pltpu.VMEM((depth, batch), BF16),
            pltpu.VMEM((batch, width), BF16),
            pltpu.VMEM((batch, depth), BF16),
            pltpu.VMEM((3, depth, width), BF16),
            pltpu.VMEM((3, pairs, block, width), BF16),
            pltpu.VMEM((3, max(pairs - 1, 1), block, width), BF16),
            pltpu.VMEM((3, block, width), BF16),
            pltpu.VMEM((2, 8, LANES), F32),
            pltpu.VMEM((n, 3, 8, LANES), F32),
            pltpu.VMEM((c, 2, 8, LANES), F32),
            pltpu.VMEM((n, 3, 8, LANES), F32),
            pltpu.SemaphoreType.DMA((7,)),
            pltpu.SemaphoreType.DMA((copies,)),
            pltpu.SemaphoreType.DMA((copies,)),
        ],
        compiler_params=pltpu.CompilerParams(
            collective_id=0, has_side_effects=True, vmem_limit_bytes=63 * 1024 * 1024
        ),
    )(
        images_in,
        images_mid,
        jnp.swapaxes(images_out, 1, 2),
        ends_in,
        ends_mid,
        jnp.swapaxes(ends_out, 1, 2),
        data_pool,
        batch_rows,
        labels,
        climbing,
    )
    return (outs[0], outs[1], jnp.swapaxes(outs[2], 1, 2), *outs[3:])


def solution(mesh):
    placed = (
        P("chain", "dp", None),
        P("chain", "dp", None),
        P("chain", "dp", None),
        P(None, "dp", None),
        P(None, "dp", None),
        P(None, "dp", None),
        P("dp", None),
        P("chain", "dp"),
        P("chain", "dp"),
        P("chain"),
    )
    return jax.shard_map(
        functools.partial(on_device, mesh.shape["dp"], mesh.shape["chain"]),
        mesh=mesh,
        in_specs=placed,
        out_specs=(
            P("chain", "dp", None),
            P("chain", "dp", None),
            P("chain", "dp", None),
            P("chain"),
            P("chain"),
            P("chain"),
        ),
        check_vma=False,
    )
```
